8 devices in a mesh: batch: 1 (over z), cols: 2 (over y), rows: 4 (over x, core).
Axes of the slice: x: 2, y: 2, z: 1, core: 2. Of those that a mesh axis runs over, the one named last changes fastest.
Arguments:
- frames: bfloat16 [4, 2, 64, 16, 384], P(None, 'batch', 'rows', 'cols')
- w_x: bfloat16 [3, 3, 384, 1536], replicated
- w_h: bfloat16 [3, 3, 384, 1536], replicated
- gate_bias: float32 [1536], replicated
- h_init: bfloat16 [2, 64, 16, 384], P('batch', 'rows', 'cols')
- c_init: float32 [2, 64, 16, 384], P('batch', 'rows', 'cols')
Outputs:
- output 1: bfloat16 [4, 2, 64, 16, 384], P(None, 'batch', 'rows', 'cols')
- output 2: float32 [2, 64, 16, 384], P('batch', 'rows', 'cols')
All inputs are finite; a program needn't handle non-finite values.
Results may differ from the reference program's by a relative error of at most 0.001.
Values are sent between devices in bfloat16 or wider.
A program may use at most 1 GiB of HBM per device.

```python
import jax
import jax.numpy as jnp
from jax import lax

STEPS = 4
SAMPLES = 2
GRID_HEIGHT = 64
GRID_WIDTH = 16
IN_CHANNELS = 384
HIDDEN = 384
BAND_ROWS = 8


def setup_inputs(seed: int = 0, part: int = 0) -> dict:
    root_key = jax.random.key(seed)
    shared_key, local_root = jax.random.split(root_key)
    local_key = jax.random.fold_in(local_root, part)
    key_wx, key_wh, key_bias = jax.random.split(shared_key, 3)
    key_frames, key_hidden, key_cell = jax.random.split(local_key, 3)
    gate_width = 4 * HIDDEN
    frames = jax.random.normal(key_frames, (STEPS, SAMPLES, GRID_HEIGHT, GRID_WIDTH, IN_CHANNELS), jnp.float32)
    w_x = jax.random.normal(key_wx, (3, 3, IN_CHANNELS, gate_width), jnp.float32) * (0.8 * (9 * IN_CHANNELS) ** -0.5)
    w_h = jax.random.normal(key_wh, (3, 3, HIDDEN, gate_width), jnp.float32) * (1.5 * (9 * HIDDEN) ** -0.5)
    forget_shift = jnp.concatenate([jnp.zeros((HIDDEN,), jnp.float32), jnp.ones((HIDDEN,), jnp.float32), jnp.zeros((2 * HIDDEN,), jnp.float32)])
    gate_bias = 0.5 * jax.random.normal(key_bias, (gate_width,), jnp.float32) + forget_shift
    h_init = 0.5 * jax.random.normal(key_hidden, (SAMPLES, GRID_HEIGHT, GRID_WIDTH, HIDDEN), jnp.float32)
    c_init = jax.random.normal(key_cell, (SAMPLES, GRID_HEIGHT, GRID_WIDTH, HIDDEN), jnp.float32)
    return {"frames": frames.astype(jnp.bfloat16), "w_x": w_x.astype(jnp.bfloat16), "w_h": w_h.astype(jnp.bfloat16), "gate_bias": gate_bias, "h_init": h_init.astype(jnp.bfloat16), "c_init": c_init}


def conv_taps(padded, weights, out_rows, out_cols):
    tap_list = [padded[:, row_off:row_off + out_rows, col_off:col_off + out_cols, :] for row_off in range(3) for col_off in range(3)]
    patches = jnp.concatenate(tap_list, axis=-1)
    flat_patches = patches.reshape(-1, patches.shape[-1])
    flat_weights = weights.reshape(-1, weights.shape[-1])
    product = jnp.dot(flat_patches, flat_weights, preferred_element_type=jnp.float32)
    return product.reshape(padded.shape[0], out_rows, out_cols, -1)


def lstm_cell(gate_sum, cell_prev):
    hidden_width = cell_prev.shape[-1]
    in_gate = jax.nn.sigmoid(gate_sum[..., :hidden_width])
    forget_gate = jax.nn.sigmoid(gate_sum[..., hidden_width:2 * hidden_width])
    out_gate = jax.nn.sigmoid(gate_sum[..., 2 * hidden_width:3 * hidden_width])
    cand_gate = jnp.tanh(gate_sum[..., 3 * hidden_width:])
    cell_next = forget_gate * cell_prev + in_gate * cand_gate
    hidden_next = (out_gate * jnp.tanh(cell_next)).astype(jnp.bfloat16)
    return hidden_next, cell_next


def reference(frames, w_x, w_h, gate_bias, h_init, c_init):
    num_bands = GRID_HEIGHT // BAND_ROWS
    pad_cfg = ((0, 0), (1, 1), (1, 1), (0, 0))

    def step_fn(state_pair, frame_t):
        hidden, cell_state = state_pair
        frame_pad = jnp.pad(frame_t, pad_cfg)
        hidden_pad = jnp.pad(hidden, pad_cfg)

        def band_update(band_index):
            row_start = band_index * BAND_ROWS
            frame_band = lax.dynamic_slice_in_dim(frame_pad, row_start, BAND_ROWS + 2, axis=1)
            hidden_band = lax.dynamic_slice_in_dim(hidden_pad, row_start, BAND_ROWS + 2, axis=1)
            cell_band = lax.dynamic_slice_in_dim(cell_state, row_start, BAND_ROWS, axis=1)
            gate_sum = conv_taps(frame_band, w_x, BAND_ROWS, GRID_WIDTH) + conv_taps(hidden_band, w_h, BAND_ROWS, GRID_WIDTH) + gate_bias
            return lstm_cell(gate_sum, cell_band)

        band_hidden, band_cell = lax.map(band_update, jnp.arange(num_bands))
        hidden_next = jnp.moveaxis(band_hidden, 0, 1).reshape(SAMPLES, GRID_HEIGHT, GRID_WIDTH, HIDDEN)
        cell_next = jnp.moveaxis(band_cell, 0, 1).reshape(SAMPLES, GRID_HEIGHT, GRID_WIDTH, HIDDEN)
        return (hidden_next, cell_next), hidden_next

    final_pair, all_hidden = lax.scan(step_fn, (h_init, c_init), frames)
    return all_hidden, final_pair[1]
```

```python
import functools

import jax
import jax.numpy as jnp
from jax import lax
from jax.experimental import pallas as pl
from jax.experimental.pallas import tpu as pltpu
from jax.sharding import PartitionSpec as P

MESH = pl.DeviceIdType.MESH
BF16 = jnp.bfloat16
F32 = jnp.float32

STEPS = 4
SEQS = 2
ROWS = 16
COLS = 8
CH = 384
LANES = 128
CHUNKS = CH // LANES
TAP_ROWS = 3 * CH
DEPTH = 3 * TAP_ROWS
GATES = 4 * CH
CELLS = ROWS * SEQS * COLS
PITCH = 16
GROUPS = (ROWS + 2) * SEQS
STAGE_ROWS = GROUPS * PITCH + 8


def sigmoid(value):
    return 0.5 * jnp.tanh(0.5 * value) + 0.5


def im2col(taps):
    return jnp.concatenate([taps[d * 16 : d * 16 + CELLS, :] for d in range(3)], axis=1)


def gate_columns(weights, block):
    return jnp.concatenate([weights[:, g * CH + block * LANES : g * CH + (block + 1) * LANES] for g in range(4)], axis=1)


def kernel(
    row_count,
    frames_hbm, wx_hbm, wh_hbm, bias_ref, h_hbm, c_hbm,
    out_hbm, c_out_hbm,
    wx, wh, frames, hidden, cell, xtaps, htaps, gate_x, stage,
    send_col, send_cor, recv_row, recv_col, recv_cor,
    in_sem, w_sem, out_sem, send_sem, recv_sem,
):
    row = lax.axis_index("rows")
    col = lax.axis_index("cols")
    other = 1 - col
    has_up = row > 0
    has_down = row < row_count - 1
    first_col = col == 0

    loads = []
    for t in range(STEPS):
        loads.append([pltpu.make_async_copy(frames_hbm.at[t, s], frames.at[t, :, s], in_sem.at[t, s]) for s in range(SEQS)])
    loads.append([pltpu.make_async_copy(h_hbm.at[s], hidden.at[0, :, s], in_sem.at[STEPS, s]) for s in range(SEQS)])
    loads.append([pltpu.make_async_copy(c_hbm.at[s], cell.at[:, s], in_sem.at[STEPS + 1, s]) for s in range(SEQS)])
    w_loads = [pltpu.make_async_copy(src, dst, w_sem.at[i]) for i, (src, dst) in enumerate(((wx_hbm, wx), (wh_hbm, wh)))]
    for group in (loads[0], loads[STEPS], loads[1], loads[2], loads[3]):
        for copy in group:
            copy.start()
    w_loads[0].start()
    for copy in loads[STEPS + 1]:
        copy.start()
    w_loads[1].start()

    recv_row[...] = jnp.zeros_like(recv_row)
    recv_cor[...] = jnp.zeros_like(recv_cor)

    barrier = pltpu.get_barrier_semaphore()

    def greet(r, c):
        pl.semaphore_signal(barrier, inc=1, device_id={"rows": r, "cols": c}, device_id_type=MESH)

    greet(row, other)

    @pl.when(has_up)
    def _():
        greet(row - 1, col)
        greet(row - 1, other)

    @pl.when(has_down)
    def _():
        greet(row + 1, col)
        greet(row + 1, other)

    inner = jnp.logical_and(has_up, has_down)

    @pl.when(inner)
    def _():
        pl.semaphore_wait(barrier, 5)

    @pl.when(jnp.logical_not(inner))
    def _():
        pl.semaphore_wait(barrier, 3)

    def tile_ref(field):
        return frames.at[field] if field < STEPS else hidden.at[field - STEPS]

    def remote(field, k, src, dst, r, c):
        return pltpu.make_async_remote_copy(
            src_ref=src, dst_ref=dst, send_sem=send_sem.at[field, k], recv_sem=recv_sem.at[field, k],
            device_id={"rows": r, "cols": c}, device_id_type=MESH,
        )

    def copies(field):
        tile = tile_ref(field)
        return dict(
            up=remote(field, 0, tile.at[0], recv_row.at[field, 1], row - 1, col),
            down=remote(field, 1, tile.at[ROWS - 1], recv_row.at[field, 0], row + 1, col),
            side=remote(field, 2, send_col.at[field], recv_col.at[field], row, other),
            up_side=remote(field, 3, send_cor.at[field, 0], recv_cor.at[field, 1], row - 1, other),
            down_side=remote(field, 4, send_cor.at[field, 1], recv_cor.at[field, 0], row + 1, other),
        )

    def send(field):
        out = copies(field)

        @pl.when(has_up)
        def _():
            out["up_side"].start()
            out["up"].start()

        @pl.when(has_down)
        def _():
            out["down_side"].start()
            out["down"].start()

        out["side"].start()

    def wait_recv(field):
        out = copies(field)
        out["side"].wait_recv()

        @pl.when(has_down)
        def _():
            out["up_side"].wait_recv()
            out["up"].wait_recv()

        @pl.when(has_up)
        def _():
            out["down_side"].wait_recv()
            out["down"].wait_recv()

    def wait_send(field):
        out = copies(field)
        out["side"].wait_send()

        @pl.when(has_up)
        def _():
            out["up_side"].wait_send()
            out["up"].wait_send()

        @pl.when(has_down)
        def _():
            out["down_side"].wait_send()
            out["down"].wait_send()

    def stage_tile(values, k, slot):
        for g in range(ROWS * SEQS):
            stage[slot, k, pl.ds((g + SEQS) * PITCH + 8, 8), :] = values[g]

    def edge_column(field, k, slot):
        start = SEQS * PITCH + 8
        last = stage[slot, k, pl.ds(start + COLS - 1, ROWS * SEQS, stride=PITCH), :]
        first = stage[slot, k, pl.ds(start, ROWS * SEQS, stride=PITCH), :]
        edge = jnp.where(first_col, last, first).astype(BF16)
        lanes = pl.ds(k * LANES, LANES)
        send_col[field, :, lanes] = edge
        send_cor[field, 0, :, lanes] = edge[:SEQS]
        send_cor[field, 1, :, lanes] = edge[-SEQS:]

    def build(field, taps, slot):
        for k in range(CHUNKS):
            lanes = pl.ds(k * LANES, LANES)
            for side, g0 in ((0, 0), (1, GROUPS - SEQS)):
                for s in range(SEQS):
                    stage[slot, k, pl.ds((g0 + s) * PITCH + 8, 8), :] = recv_row[field, side, s, :, lanes].astype(F32)
            pieces = ((recv_cor[field, 0, :, lanes], 0, SEQS), (recv_col[field, :, lanes], SEQS, ROWS * SEQS), (recv_cor[field, 1, :, lanes], GROUPS - SEQS, SEQS))
            for value, g0, count in pieces:
                value = value.astype(F32)
                stage[slot, k, pl.ds(g0 * PITCH + 7, count, stride=PITCH), :] = jnp.where(first_col, 0.0, value)
                stage[slot, k, pl.ds(g0 * PITCH + 16, count, stride=PITCH), :] = jnp.where(first_col, value, 0.0)
            for y in range(ROWS + 2):
                for d in range(3):
                    pair = [stage[slot, k, pl.ds((y * SEQS + s) * PITCH + 7 + d, 8), :] for s in range(SEQS)]
                    taps[y * 16 : (y + 1) * 16, d * CH + k * LANES : d * CH + (k + 1) * LANES] = jnp.concatenate(pair, axis=0).astype(BF16)

    def prepare(field, slot):
        tile = tile_ref(field)
        for k in range(CHUNKS):
            values = tile[:, :, :, k * LANES : (k + 1) * LANES].astype(F32).reshape(ROWS * SEQS, 8, LANES)
            stage_tile(values, k, slot)
            edge_column(field, k, slot)

    for field, group in ((0, loads[0]), (STEPS, loads[STEPS]), (1, loads[1]), (2, loads[2]), (3, loads[3])):
        for copy in group:
            copy.wait()
        prepare(field, min(field, STEPS))
        send(field)

    def conv_x(t):
        lhs = im2col(xtaps)
        for block in range(CHUNKS):
            gate_x[block] = jnp.dot(lhs, gate_columns(wx, block), preferred_element_type=F32)

    w_loads[0].wait()
    wait_recv(0)
    build(0, xtaps, 0)
    conv_x(0)
    for copy in loads[STEPS + 1]:
        copy.wait()
    w_loads[1].wait()
    wait_recv(STEPS)
    build(STEPS, htaps, STEPS)

    outs = []
    for t in range(STEPS):
        lhs = im2col(htaps)
        for block in range(CHUNKS):
            lanes = slice(block * LANES, (block + 1) * LANES)
            sums = jnp.dot(lhs, gate_columns(wh, block), preferred_element_type=F32) + gate_x[block]
            gates = [sums[:, g * LANES : (g + 1) * LANES] + bias_ref[:, g * CH + block * LANES : g * CH + (block + 1) * LANES] for g in range(4)]
            shape = (ROWS, SEQS, COLS, LANES)
            c_old = cell[:, :, :, lanes].reshape(CELLS, LANES)
            c_new = sigmoid(gates[1]) * c_old + sigmoid(gates[0]) * jnp.tanh(gates[3])
            h_new = sigmoid(gates[2]) * jnp.tanh(c_new)
            cell[:, :, :, lanes] = c_new.reshape(shape)
            hidden[t + 1, :, :, :, lanes] = h_new.reshape(shape).astype(BF16)
            if t + 1 < STEPS:
                stage_tile(h_new.reshape(ROWS * SEQS, 8, LANES), block, STEPS)
                edge_column(STEPS + t + 1, block, STEPS)
        if t + 1 < STEPS:
            send(STEPS + t + 1)
        for s in range(SEQS):
            outs.append(pltpu.make_async_copy(hidden.at[t + 1, :, s], out_hbm.at[t, s], out_sem.at[t, s]))
            outs[-1].start()
        if t + 1 < STEPS:
            wait_recv(t + 1)
            build(t + 1, xtaps, t + 1)
            conv_x(t + 1)
            wait_recv(STEPS + t + 1)
            build(STEPS + t + 1, htaps, STEPS)
    for s in range(SEQS):
        outs.append(pltpu.make_async_copy(cell.at[:, s], c_out_hbm.at[s], out_sem.at[STEPS, s]))
        outs[-1].start()
    for field in range(2 * STEPS):
        wait_send(field)
    for copy in outs:
        copy.wait()


def solution(mesh):
    row_count = mesh.shape["rows"]
    frame_spec = P(None, "batch", "rows", "cols", None)
    state_spec = P("batch", "rows", "cols", None)

    def local_run(frames, w_x, w_h, gate_bias, h_init, c_init):
        any_space = pl.BlockSpec(memory_space=pl.ANY)
        vmem = pl.BlockSpec(memory_space=pltpu.VMEM)
        fields = 2 * STEPS
        return pl.pallas_call(
            functools.partial(kernel, row_count),
            out_shape=(jax.ShapeDtypeStruct(frames.shape, BF16), jax.ShapeDtypeStruct(c_init.shape, F32)),
            in_specs=[any_space, any_space, any_space, vmem, any_space, any_space],
            out_specs=(any_space, any_space),
            scratch_shapes=[
                pltpu.VMEM((DEPTH, GATES), BF16),
                pltpu.VMEM((DEPTH, GATES), BF16),
                pltpu.VMEM((STEPS, ROWS, SEQS, COLS, CH), BF16),
                pltpu.VMEM((STEPS + 1, ROWS, SEQS, COLS, CH), BF16),
                pltpu.VMEM((ROWS, SEQS, COLS, CH), F32),
                pltpu.VMEM(((ROWS + 2) * 16, TAP_ROWS), BF16),
                pltpu.VMEM(((ROWS + 2) * 16, TAP_ROWS), BF16),
                pltpu.VMEM((CHUNKS, CELLS, 4 * LANES), F32),
                pltpu.VMEM((STEPS + 1, CHUNKS, STAGE_ROWS, LANES), F32),
                pltpu.VMEM((fields, ROWS * SEQS, CH), BF16),
                pltpu.VMEM((fields, 2, SEQS, CH), BF16),
                pltpu.VMEM((fields, 2, SEQS, COLS, CH), BF16),
                pltpu.VMEM((fields, ROWS * SEQS, CH), BF16),
                pltpu.VMEM((fields, 2, SEQS, CH), BF16),
                pltpu.SemaphoreType.DMA((STEPS + 2, SEQS)),
                pltpu.SemaphoreType.DMA((2,)),
                pltpu.SemaphoreType.DMA((STEPS + 1, SEQS)),
                pltpu.SemaphoreType.DMA((fields, 5)),
                pltpu.SemaphoreType.DMA((fields, 5)),
            ],
            compiler_params=pltpu.CompilerParams(collective_id=0, has_side_effects=True, vmem_limit_bytes=62 * 2**20),
        )(frames, w_x.reshape(DEPTH, GATES), w_h.reshape(DEPTH, GATES), gate_bias.reshape(1, GATES), h_init, c_init)

    return jax.shard_map(local_run, mesh=mesh, in_specs=(frame_spec, P(), P(), P(), state_spec, state_spec), out_specs=(frame_spec, state_spec), check_vma=False)
```

```python
import functools

import jax
import jax.numpy as jnp
from jax import lax
from jax.experimental import pallas as pl
from jax.experimental.pallas import tpu as pltpu
from jax.sharding import PartitionSpec as P

MESH = pl.DeviceIdType.MESH
BF16 = jnp.bfloat16
F32 = jnp.float32

STEPS = 4
SEQS = 2
ROWS = 16
COLS = 8
CH = 384
LANES = 128
CHUNKS = CH // LANES
TAP_ROWS = 3 * CH
DEPTH = 3 * TAP_ROWS
GATES = 4 * CH
CELLS = ROWS * SEQS * COLS
PITCH = 16
GROUPS = (ROWS + 2) * SEQS
STAGE_ROWS = GROUPS * PITCH + 8
CENTER = 4


def sigmoid(value):
    return 0.5 * jnp.tanh(0.5 * value) + 0.5


def halves(source, taps):
    return [(source, tap, k) for tap in taps for k in range(CHUNKS)]


def kernel(
    row_count,
    frames_hbm, wx_hbm, wh_hbm, bias_hbm, h_hbm, c_hbm,
    hidden_out, cell,
    wx, wh, bias, frames, h_start, xtaps, htaps, gates, stage,
    send_col, send_cor, recv_row, recv_col, recv_cor,
    in_sem, w_sem, send_sem, recv_sem,
):
    row = lax.axis_index("rows")
    col = lax.axis_index("cols")
    other = 1 - col
    has_up = row > 0
    has_down = row < row_count - 1
    first_col = col == 0

    frame_loads = [[pltpu.make_async_copy(frames_hbm.at[t, s], frames.at[t, :, s], in_sem.at[t, s]) for s in range(SEQS)] for t in range(STEPS)]
    h_loads = [pltpu.make_async_copy(h_hbm.at[s], h_start.at[:, s], in_sem.at[STEPS, s]) for s in range(SEQS)]
    c_loads = [pltpu.make_async_copy(c_hbm.at[s], cell.at[:, s], in_sem.at[STEPS + 1, s]) for s in range(SEQS)]
    bias_load = pltpu.make_async_copy(bias_hbm, bias, w_sem.at[0, 3])
    spans = (pl.ds(CENTER * CH, CH), pl.ds(0, CENTER * CH), pl.ds((CENTER + 1) * CH, DEPTH - (CENTER + 1) * CH))
    x_loads, w_loads = [[pltpu.make_async_copy(src.at[span], dst.at[span], w_sem.at[i, n]) for n, span in enumerate(spans)] for i, (src, dst) in enumerate(((wx_hbm, wx), (wh_hbm, wh)))]
    for copy in (*frame_loads[0], *h_loads, x_loads[0], w_loads[0], *frame_loads[1], *frame_loads[2], *frame_loads[3], *x_loads[1:], *c_loads, bias_load, *w_loads[1:]):
        copy.start()

    recv_row[...] = jnp.zeros_like(recv_row)
    recv_cor[...] = jnp.zeros_like(recv_cor)

    barrier = pltpu.get_barrier_semaphore()

    def greet(r, c):
        pl.semaphore_signal(barrier, inc=1, device_id={"rows": r, "cols": c}, device_id_type=MESH)

    greet(row, other)

    @pl.when(has_up)
    def _():
        greet(row - 1, col)
        greet(row - 1, other)

    @pl.when(has_down)
    def _():
        greet(row + 1, col)
        greet(row + 1, other)

    def greeted():
        inner = jnp.logical_and(has_up, has_down)

        @pl.when(inner)
        def _():
            pl.semaphore_wait(barrier, 5)

        @pl.when(jnp.logical_not(inner))
        def _():
            pl.semaphore_wait(barrier, 3)

    def tile_ref(field):
        if field < STEPS:
            return frames.at[field]
        return h_start if field == STEPS else hidden_out.at[field - STEPS - 1]

    def remote(field, k, src, dst, r, c):
        return pltpu.make_async_remote_copy(
            src_ref=src, dst_ref=dst, send_sem=send_sem.at[field, k], recv_sem=recv_sem.at[field, k],
            device_id={"rows": r, "cols": c}, device_id_type=MESH,
        )

    def copies(field):
        tile = tile_ref(field)
        return dict(
            up=remote(field, 0, tile.at[0], recv_row.at[field, 1], row - 1, col),
            down=remote(field, 1, tile.at[ROWS - 1], recv_row.at[field, 0], row + 1, col),
            side=remote(field, 2, send_col.at[field], recv_col.at[field], row, other),
            up_side=remote(field, 3, send_cor.at[field, 0], recv_cor.at[field, 1], row - 1, other),
            down_side=remote(field, 4, send_cor.at[field, 1], recv_cor.at[field, 0], row + 1, other),
        )

    def send(field):
        out = copies(field)

        @pl.when(has_up)
        def _():
            out["up_side"].start()
            out["up"].start()

        @pl.when(has_down)
        def _():
            out["down_side"].start()
            out["down"].start()

        out["side"].start()

    def wait_recv(field):
        out = copies(field)
        out["side"].wait_recv()

        @pl.when(has_down)
        def _():
            out["up_side"].wait_recv()
            out["up"].wait_recv()

        @pl.when(has_up)
        def _():
            out["down_side"].wait_recv()
            out["down"].wait_recv()

    def wait_send(field):
        out = copies(field)
        out["side"].wait_send()

        @pl.when(has_up)
        def _():
            out["up_side"].wait_send()
            out["up"].wait_send()

        @pl.when(has_down)
        def _():
            out["down_side"].wait_send()
            out["down"].wait_send()

    def shift_lanes(d, k):
        return slice(d * CH + k * LANES, d * CH + (k + 1) * LANES)

    def field_taps(field):
        return xtaps if field < STEPS else htaps.at[field % 2]

    def own_tile(field, values, k, taps, slot):
        for g in range(ROWS * SEQS):
            stage[slot, k, pl.ds((g + SEQS) * PITCH + 8, 8), :] = values[g]
        if taps is not None:
            taps[16 : 16 + CELLS, shift_lanes(1, k)] = values.reshape(CELLS, LANES).astype(BF16)
        start = SEQS * PITCH + 8
        last = stage[slot, k, pl.ds(start + COLS - 1, ROWS * SEQS, stride=PITCH), :]
        first = stage[slot, k, pl.ds(start, ROWS * SEQS, stride=PITCH), :]
        edge = jnp.where(first_col, last, first).astype(BF16)
        lanes = pl.ds(k * LANES, LANES)
        send_col[field, :, lanes] = edge
        send_cor[field, 0, :, lanes] = edge[:SEQS]
        send_cor[field, 1, :, lanes] = edge[-SEQS:]

    def prepare(field, taps, slot):
        tile = tile_ref(field)
        for k in range(CHUNKS):
            values = tile[:, :, :, k * LANES : (k + 1) * LANES].astype(F32).reshape(ROWS * SEQS, 8, LANES)
            own_tile(field, values, k, taps, slot)

    def build(field, taps, slot, own_done):
        for k in range(CHUNKS):
            lanes = pl.ds(k * LANES, LANES)
            for side, g0 in ((0, 0), (1, GROUPS - SEQS)):
                for s in range(SEQS):
                    stage[slot, k, pl.ds((g0 + s) * PITCH + 8, 8), :] = recv_row[field, side, s, :, lanes].astype(F32)
            pieces = ((recv_cor[field, 0, :, lanes], 0, SEQS), (recv_col[field, :, lanes], SEQS, ROWS * SEQS), (recv_cor[field, 1, :, lanes], GROUPS - SEQS, SEQS))
            for value, g0, count in pieces:
                value = value.astype(F32)
                stage[slot, k, pl.ds(g0 * PITCH + 7, count, stride=PITCH), :] = jnp.where(first_col, 0.0, value)
                stage[slot, k, pl.ds(g0 * PITCH + 16, count, stride=PITCH), :] = jnp.where(first_col, value, 0.0)
            for y in range(ROWS + 2):
                for d in range(3):
                    if own_done and d == 1 and 1 <= y <= ROWS:
                        continue
                    pair = [stage[slot, k, pl.ds((y * SEQS + s) * PITCH + 7 + d, 8), :] for s in range(SEQS)]
                    taps[y * 16 : (y + 1) * 16, shift_lanes(d, k)] = jnp.concatenate(pair, axis=0).astype(BF16)

    def operand(half, t):
        source, tap, k = half
        taps = field_taps(t if source == "x" else STEPS + t)
        dy, dx = divmod(tap, 3)
        return taps[dy * 16 : dy * 16 + CELLS, shift_lanes(dx, k)]

    def weight(half, block):
        source, tap, k = half
        w = wx if source == "x" else wh
        first = tap * CH + k * LANES
        return jnp.concatenate([w[first : first + LANES, g * CH + block * LANES : g * CH + (block + 1) * LANES] for g in range(4)], axis=1)

    def product(t, block, parts):
        lhs = jnp.concatenate([operand(p, t) for p in parts], axis=1)
        rhs = jnp.concatenate([weight(p, block) for p in parts], axis=0)
        return jnp.dot(lhs, rhs, preferred_element_type=F32)

    around = [tap for tap in range(9) if tap != CENTER]
    x_part = halves("x", around)
    h_part = halves("h", around)
    own_part = halves("x", [CENTER]) + halves("h", [CENTER])

    def cell_update(t, block):
        lanes = slice(block * LANES, (block + 1) * LANES)
        sums = product(t, block, h_part) + gates[block]
        pre = [sums[:, g * LANES : (g + 1) * LANES] + bias[pl.ds(g * CH + block * LANES, LANES)] for g in range(4)]
        shape = (ROWS, SEQS, COLS, LANES)
        c_old = cell[:, :, :, lanes].reshape(CELLS, LANES)
        c_new = sigmoid(pre[1]) * c_old + sigmoid(pre[0]) * jnp.tanh(pre[3])
        h_new = sigmoid(pre[2]) * jnp.tanh(c_new)
        cell[:, :, :, lanes] = c_new.reshape(shape)
        hidden_out[t, :, :, :, lanes] = h_new.reshape(shape).astype(BF16)
        if t + 1 < STEPS:
            own_tile(STEPS + t + 1, h_new.reshape(ROWS * SEQS, 8, LANES), block, field_taps(STEPS + t + 1), STEPS)

    for field, group in ((0, frame_loads[0]), (STEPS, h_loads)):
        for copy in group:
            copy.wait()
        prepare(field, field_taps(field), field)
    greeted()
    send(0)
    send(STEPS)
    x_loads[0].wait()
    w_loads[0].wait()
    for block in range(CHUNKS):
        gates[block] = product(0, block, own_part)
    for t in range(1, STEPS):
        for copy in frame_loads[t]:
            copy.wait()
        prepare(t, None, t)
        send(t)
    for copy in (*x_loads[1:], *c_loads, bias_load):
        copy.wait()
    wait_recv(0)
    build(0, xtaps, 0, True)
    for block in range(CHUNKS):
        gates[block] += product(0, block, x_part)
    for copy in w_loads[1:]:
        copy.wait()
    wait_recv(STEPS)
    build(STEPS, field_taps(STEPS), STEPS, True)

    for t in range(STEPS):
        for block in range(CHUNKS):
            cell_update(t, block)
        if t + 1 < STEPS:
            send(STEPS + t + 1)
            wait_recv(t + 1)
            build(t + 1, xtaps, t + 1, False)
            for block in range(CHUNKS):
                gates[block] = product(t + 1, block, x_part + own_part)
            wait_recv(STEPS + t + 1)
            build(STEPS + t + 1, field_taps(STEPS + t + 1), STEPS, True)
    for field in range(2 * STEPS):
        wait_send(field)


def write_out(hidden, cell, out_hbm, c_out_hbm, sem):
    copies = [pltpu.make_async_copy(hidden.at[t, :, s], out_hbm.at[t, s], sem.at[t, s]) for t in range(STEPS) for s in range(SEQS)]
    copies += [pltpu.make_async_copy(cell.at[:, s], c_out_hbm.at[s], sem.at[STEPS, s]) for s in range(SEQS)]
    for copy in copies:
        copy.start()
    for copy in copies:
        copy.wait()


def solution(mesh):
    row_count = mesh.shape["rows"]
    frame_spec = P(None, "batch", "rows", "cols", None)
    state_spec = P("batch", "rows", "cols", None)

    def local_run(frames, w_x, w_h, gate_bias, h_init, c_init):
        hbm = pl.BlockSpec(memory_space=pltpu.HBM)
        vmem = pl.BlockSpec(memory_space=pltpu.VMEM)
        fields = 2 * STEPS
        tile = (ROWS, SEQS, COLS, CH)

        hidden, cell = pl.pallas_call(
            functools.partial(kernel, row_count),
            out_shape=(pltpu.VMEM((STEPS,) + tile, BF16), pltpu.VMEM(tile, F32)),
            in_specs=[hbm] * 6,
            out_specs=(vmem, vmem),
            scratch_shapes=[
                pltpu.VMEM((DEPTH, GATES), BF16),
                pltpu.VMEM((DEPTH, GATES), BF16),
                pltpu.VMEM((GATES,), F32),
                pltpu.VMEM((STEPS,) + tile, BF16),
                pltpu.VMEM(tile, BF16),
                pltpu.VMEM(((ROWS + 2) * 16, TAP_ROWS), BF16),
                pltpu.VMEM((2, (ROWS + 2) * 16, TAP_ROWS), BF16),
                pltpu.VMEM((CHUNKS, CELLS, 4 * LANES), F32),
                pltpu.VMEM((STEPS + 1, CHUNKS, STAGE_ROWS, LANES), F32),
                pltpu.VMEM((fields, ROWS * SEQS, CH), BF16),
                pltpu.VMEM((fields, 2, SEQS, CH), BF16),
                pltpu.VMEM((fields, 2, SEQS, COLS, CH), BF16),
                pltpu.VMEM((fields, ROWS * SEQS, CH), BF16),
                pltpu.VMEM((fields, 2, SEQS, CH), BF16),
                pltpu.SemaphoreType.DMA((STEPS + 2, SEQS)),
                pltpu.SemaphoreType.DMA((2, 4)),
                pltpu.SemaphoreType.DMA((fields, 5)),
                pltpu.SemaphoreType.DMA((fields, 5)),
            ],
            compiler_params=pltpu.CompilerParams(collective_id=0, has_side_effects=True, vmem_limit_bytes=48 * 2**20),
        )(*(pltpu.with_memory_space_constraint(a, pltpu.HBM) for a in (frames, w_x.reshape(DEPTH, GATES), w_h.reshape(DEPTH, GATES), gate_bias, h_init, c_init)))
        return pl.pallas_call(
            write_out,
            out_shape=(jax.ShapeDtypeStruct(frames.shape, BF16), jax.ShapeDtypeStruct(c_init.shape, F32)),
            in_specs=[vmem, vmem],
            out_specs=(hbm, hbm),
            scratch_shapes=[pltpu.SemaphoreType.DMA((STEPS + 1, SEQS))],
        )(*(pltpu.with_memory_space_constraint(a, pltpu.VMEM) for a in (hidden, cell)))

    return jax.shard_map(local_run, mesh=mesh, in_specs=(frame_spec, P(), P(), P(), state_spec, state_spec), out_specs=(frame_spec, state_spec), check_vma=False)
```

```python
import functools

import jax
import jax.numpy as jnp
from jax import lax
from jax.experimental import pallas as pl
from jax.experimental.pallas import tpu as pltpu
from jax.sharding import PartitionSpec as P

MESH = pl.DeviceIdType.MESH
BF16 = jnp.bfloat16
F32 = jnp.float32

STEPS = 4
SEQS = 2
ROWS = 16
COLS = 8
CH = 384
LANES = 128
CHUNKS = CH // LANES
TAP_ROWS = 3 * CH
DEPTH = 3 * TAP_ROWS
GATES = 4 * CH
CELLS = ROWS * SEQS * COLS
PITCH = 16
GROUPS = (ROWS + 2) * SEQS
STAGE_ROWS = GROUPS * PITCH + 8
OWN = (4,)
VERTICAL = (1, 7)
SIDE = (0, 2, 3, 5, 6, 8)


def sigmoid(value):
    return 0.5 * jnp.tanh(0.5 * value) + 0.5


def halves(source, taps):
    return [(source, tap, k) for tap in taps for k in range(CHUNKS)]


def kernel(
    row_count,
    frames_hbm, wx_hbm, wh_hbm, bias_hbm, h_hbm, c_hbm,
    hidden_out, cell,
    wx, wh, bias, frames, h_start, xtaps, htaps, gates, stage,
    send_col, send_cor, recv_row, recv_col, recv_cor,
    load_sem, send_sem, recv_sem,
):
    row = lax.axis_index("rows")
    col = lax.axis_index("cols")
    other = 1 - col
    has_up = row > 0
    has_down = row < row_count - 1
    inner = jnp.logical_and(has_up, has_down)
    first_col = col == 0

    group_of = {}
    for name in ("frame0", "state", "own_x", "own_h", "frame1", "frames", "cell", "bias", "near_x", "far_x", "last_x", "most_h", "last_h"):
        group_of[name] = load_sem.at[len(group_of)]

    def load(name, queue, pairs):
        for src, dst in pairs:
            pltpu.make_async_copy(src, dst, group_of[name]).start(priority=queue)

    def loaded(name, whole):
        pltpu.make_async_copy(whole, whole, group_of[name]).wait()

    def frame_pairs(times):
        return [(frames_hbm.at[t, s], frames.at[t, :, s]) for t in times for s in range(SEQS)]

    def tap_pairs(src, dst, taps):
        return [(src.at[pl.ds(tap * CH, CH)], dst.at[pl.ds(tap * CH, CH)]) for tap in taps]

    def taps_like(dst, count):
        return dst.at[pl.ds(0, count * CH)]

    load("frame0", 0, frame_pairs([0]))
    load("state", 0, [(h_hbm.at[s], h_start.at[:, s]) for s in range(SEQS)])
    load("own_x", 1, tap_pairs(wx_hbm, wx, OWN))
    load("own_h", 1, tap_pairs(wh_hbm, wh, OWN))
    load("frame1", 0, frame_pairs([1]))
    load("frames", 0, frame_pairs([2, 3]))
    load("cell", 0, [(c_hbm.at[s], cell.at[:, s]) for s in range(SEQS)])
    load("bias", 0, [(bias_hbm, bias)])
    load("near_x", 1, tap_pairs(wx_hbm, wx, VERTICAL))
    load("far_x", 1, tap_pairs(wx_hbm, wx, SIDE[:4]))
    load("last_x", 1, tap_pairs(wx_hbm, wx, SIDE[4:]))
    load("most_h", 1, tap_pairs(wh_hbm, wh, VERTICAL + SIDE[:4]))
    load("last_h", 1, tap_pairs(wh_hbm, wh, SIDE[4:]))

    recv_row[...] = jnp.zeros_like(recv_row)
    recv_cor[...] = jnp.zeros_like(recv_cor)

    barrier = pltpu.get_barrier_semaphore()

    def greet(r, c):
        pl.semaphore_signal(barrier, inc=1, device_id={"rows": r, "cols": c}, device_id_type=MESH)

    greet(row, other)

    @pl.when(has_up)
    def _():
        greet(row - 1, col)
        greet(row - 1, other)

    @pl.when(has_down)
    def _():
        greet(row + 1, col)
        greet(row + 1, other)

    def greeted():
        @pl.when(inner)
        def _():
            pl.semaphore_wait(barrier, 5)

        @pl.when(jnp.logical_not(inner))
        def _():
            pl.semaphore_wait(barrier, 3)

    def tile_ref(field):
        if field < STEPS:
            return frames.at[field]
        return h_start if field == STEPS else hidden_out.at[field - STEPS - 1]

    def field_taps(field):
        return xtaps.at[field % 2] if field < STEPS else htaps.at[field % 2]

    def remote(field, n, src, dst, r, c):
        return pltpu.make_async_remote_copy(
            src_ref=src, dst_ref=dst, send_sem=send_sem.at[n], recv_sem=recv_sem.at[field, (0, 0, 1, 2, 2)[n]],
            device_id={"rows": r, "cols": c}, device_id_type=MESH,
        )

    def copies(field):
        tile = tile_ref(field)
        return dict(
            up=remote(field, 0, tile.at[0], recv_row.at[field, 1], row - 1, col),
            down=remote(field, 1, tile.at[ROWS - 1], recv_row.at[field, 0], row + 1, col),
            side=remote(field, 2, send_col.at[field], recv_col.at[field], row, other),
            up_side=remote(field, 3, send_cor.at[field, 0], recv_cor.at[field, 1], row - 1, other),
            down_side=remote(field, 4, send_cor.at[field, 1], recv_cor.at[field, 0], row + 1, other),
        )

    def send(field):
        out = copies(field)

        @pl.when(has_up)
        def _():
            out["up_side"].start()
            out["up"].start()

        @pl.when(has_down)
        def _():
            out["down_side"].start()
            out["down"].start()

        out["side"].start()

    def pair_arrived(field, n, both):
        @pl.when(inner)
        def _():
            pltpu.make_async_copy(both, both, recv_sem.at[field, n]).wait()

        @pl.when(jnp.logical_not(inner))
        def _():
            pltpu.make_async_copy(both.at[0], both.at[0], recv_sem.at[field, n]).wait()

    def rows_arrived(field):
        pair_arrived(field, 0, recv_row.at[field])

    def sides_arrived(field):
        pltpu.make_async_copy(recv_col.at[field], recv_col.at[field], recv_sem.at[field, 1]).wait()
        pair_arrived(field, 2, recv_cor.at[field])

    def all_sent():
        whole_row, whole_cor = recv_row.at[:, 0], recv_cor.at[:, 0]
        remote(0, 2, recv_col, recv_col, row, other).wait_send()

        @pl.when(has_up)
        def _():
            remote(0, 0, whole_row, whole_row, row - 1, col).wait_send()
            remote(0, 3, whole_cor, whole_cor, row - 1, other).wait_send()

        @pl.when(has_down)
        def _():
            remote(0, 1, whole_row, whole_row, row + 1, col).wait_send()
            remote(0, 4, whole_cor, whole_cor, row + 1, other).wait_send()

    def shift_lanes(d, k):
        return slice(d * CH + k * LANES, d * CH + (k + 1) * LANES)

    def slot_of(field):
        return min(field, STEPS)

    def own_tile(field, values, k):
        slot = slot_of(field)
        for g in range(ROWS * SEQS):
            stage[slot, k, pl.ds((g + SEQS) * PITCH + 8, 8), :] = values[g]
        if field == 0 or field >= STEPS:
            field_taps(field)[16 : 16 + CELLS, shift_lanes(1, k)] = values.reshape(CELLS, LANES).astype(BF16)
        begin = SEQS * PITCH + 8
        last = stage[slot, k, pl.ds(begin + COLS - 1, ROWS * SEQS, stride=PITCH), :]
        first = stage[slot, k, pl.ds(begin, ROWS * SEQS, stride=PITCH), :]
        edge = jnp.where(first_col, last, first).astype(BF16)
        lanes = pl.ds(k * LANES, LANES)
        send_col[field, :, lanes] = edge
        send_cor[field, 0, :, lanes] = edge[:SEQS]
        send_cor[field, 1, :, lanes] = edge[-SEQS:]

    def prepare(field):
        tile = tile_ref(field)
        for k in range(CHUNKS):
            values = tile[:, :, :, k * LANES : (k + 1) * LANES].astype(F32).reshape(ROWS * SEQS, 8, LANES)
            own_tile(field, values, k)

    def shifted(field, y, d, k):
        slot = slot_of(field)
        pair = [stage[slot, k, pl.ds((y * SEQS + s) * PITCH + 7 + d, 8), :] for s in range(SEQS)]
        field_taps(field)[y * 16 : (y + 1) * 16, shift_lanes(d, k)] = jnp.concatenate(pair, axis=0).astype(BF16)

    def build_rows(field):
        slot = slot_of(field)
        for k in range(CHUNKS):
            lanes = pl.ds(k * LANES, LANES)
            for side, g0 in ((0, 0), (1, GROUPS - SEQS)):
                for s in range(SEQS):
                    stage[slot, k, pl.ds((g0 + s) * PITCH + 8, 8), :] = recv_row[field, side, s, :, lanes].astype(F32)
            for y in (0, ROWS + 1) if field == 0 or field >= STEPS else range(ROWS + 2):
                shifted(field, y, 1, k)

    def build_sides(field):
        slot = slot_of(field)
        for k in range(CHUNKS):
            lanes = pl.ds(k * LANES, LANES)
            pieces = ((recv_cor[field, 0, :, lanes], 0, SEQS), (recv_col[field, :, lanes], SEQS, ROWS * SEQS), (recv_cor[field, 1, :, lanes], GROUPS - SEQS, SEQS))
            for value, g0, count in pieces:
                value = value.astype(F32)
                stage[slot, k, pl.ds(g0 * PITCH + 7, count, stride=PITCH), :] = jnp.where(first_col, 0.0, value)
                stage[slot, k, pl.ds(g0 * PITCH + 16, count, stride=PITCH), :] = jnp.where(first_col, value, 0.0)
            for y in range(ROWS + 2):
                shifted(field, y, 0, k)
                shifted(field, y, 2, k)

    def operand(half, t):
        source, tap, k = half
        taps = field_taps(t if source == "x" else STEPS + t)
        dy, dx = divmod(tap, 3)
        return taps[dy * 16 : dy * 16 + CELLS, shift_lanes(dx, k)]

    def weight(half, block):
        source, tap, k = half
        w = wx if source == "x" else wh
        first = tap * CH + k * LANES
        return jnp.concatenate([w[first : first + LANES, g * CH + block * LANES : g * CH + (block + 1) * LANES] for g in range(4)], axis=1)

    def product(t, block, parts):
        lhs = jnp.concatenate([operand(p, t) for p in parts], axis=1)
        rhs = jnp.concatenate([weight(p, block) for p in parts], axis=0)
        return jnp.dot(lhs, rhs, preferred_element_type=F32)

    def cell_update(t, block, sums):
        lanes = slice(block * LANES, (block + 1) * LANES)
        pre = [sums[:, g * LANES : (g + 1) * LANES] + bias[pl.ds(g * CH + block * LANES, LANES)] for g in range(4)]
        shape = (ROWS, SEQS, COLS, LANES)
        c_old = cell[:, :, :, lanes].reshape(CELLS, LANES)
        c_new = sigmoid(pre[1]) * c_old + sigmoid(pre[0]) * jnp.tanh(pre[3])
        h_new = sigmoid(pre[2]) * jnp.tanh(c_new)
        cell[:, :, :, lanes] = c_new.reshape(shape)
        hidden_out[t, :, :, :, lanes] = h_new.reshape(shape).astype(BF16)
        if t + 1 < STEPS:
            own_tile(STEPS + t + 1, h_new.reshape(ROWS * SEQS, 8, LANES), block)

    x_all = halves("x", VERTICAL + SIDE)
    x_own, x_vertical, x_side = (halves("x", taps) for taps in (OWN, VERTICAL, SIDE))
    h_own, h_vertical, h_side = (halves("h", taps) for taps in (OWN, VERTICAL, SIDE))

    def add(t, block, parts):
        gates[t, block] += product(t, block, parts)

    loaded("frame0", frames.at[0])
    prepare(0)
    loaded("state", h_start)
    prepare(STEPS)
    greeted()
    send(0)
    send(STEPS)
    loaded("own_x", taps_like(wx, 1))
    loaded("own_h", taps_like(wh, 1))
    loaded("frame1", frames.at[1])
    for block in range(CHUNKS):
        gates[0, block] = product(0, block, x_own + h_own)
    prepare(1)
    send(1)
    loaded("near_x", taps_like(wx, 2))
    rows_arrived(0)
    build_rows(0)
    for block in range(CHUNKS):
        add(0, block, x_vertical)
    loaded("far_x", taps_like(wx, 4))
    sides_arrived(0)
    build_sides(0)
    for block in range(CHUNKS):
        add(0, block, x_side[:12])
    loaded("last_x", taps_like(wx, 2))
    for block in range(CHUNKS):
        add(0, block, x_side[12:])
    loaded("frames", frames.at[pl.ds(2, 2)])
    rows_arrived(1)
    sides_arrived(1)
    build_rows(1)
    build_sides(1)
    for block in range(CHUNKS):
        gates[1, block] = product(1, block, x_all[:16])
    prepare(2)
    prepare(3)
    send(2)
    send(3)
    loaded("cell", cell)
    loaded("bias", bias)
    loaded("most_h", taps_like(wh, 6))
    rows_arrived(STEPS)
    sides_arrived(STEPS)
    build_rows(STEPS)
    build_sides(STEPS)
    for block in range(CHUNKS):
        add(0, block, h_vertical + h_side[:12])
    loaded("last_h", taps_like(wh, 2))
    for block in range(CHUNKS):
        cell_update(0, block, gates[0, block] + product(0, block, h_side[12:]))
    send(STEPS + 1)

    rest = {1: x_all[16:], 2: x_all[12:], 3: x_all[6:]}
    ahead = {1: x_all[:12], 2: x_all[:6]}
    for t in range(1, STEPS):
        if t in ahead:
            rows_arrived(t + 1)
            sides_arrived(t + 1)
            build_rows(t + 1)
            build_sides(t + 1)
            for block in range(CHUNKS):
                gates[t + 1, block] = product(t + 1, block, ahead[t])
        for block in range(CHUNKS):
            add(t, block, rest[t] + x_own + h_own)
        rows_arrived(STEPS + t)
        build_rows(STEPS + t)
        for block in range(CHUNKS):
            add(t, block, h_vertical)
        sides_arrived(STEPS + t)
        if t + 1 == STEPS:
            all_sent()
        build_sides(STEPS + t)
        for block in range(CHUNKS):
            cell_update(t, block, gates[t, block] + product(t, block, h_side))
        if t + 1 < STEPS:
            send(STEPS + t + 1)


def write_out(hidden, cell, out_hbm, c_out_hbm, sem):
    copies = [pltpu.make_async_copy(hidden.at[t, :, s], out_hbm.at[t, s], sem.at[t, s]) for t in range(STEPS) for s in range(SEQS)]
    copies += [pltpu.make_async_copy(cell.at[:, s], c_out_hbm.at[s], sem.at[STEPS, s]) for s in range(SEQS)]
    for copy in copies:
        copy.start()
    for copy in copies:
        copy.wait()


def solution(mesh):
    row_count = mesh.shape["rows"]
    frame_spec = P(None, "batch", "rows", "cols", None)
    state_spec = P("batch", "rows", "cols", None)

    def local_run(frames, w_x, w_h, gate_bias, h_init, c_init):
        hbm = pl.BlockSpec(memory_space=pltpu.HBM)
        vmem = pl.BlockSpec(memory_space=pltpu.VMEM)
        fields = 2 * STEPS
        tile = (ROWS, SEQS, COLS, CH)

        hidden, cell = pl.pallas_call(
            functools.partial(kernel, row_count),
            out_shape=(pltpu.VMEM((STEPS,) + tile, BF16), pltpu.VMEM(tile, F32)),
            in_specs=[hbm] * 6,
            out_specs=(vmem, vmem),
            scratch_shapes=[
                pltpu.VMEM((DEPTH, GATES), BF16),
                pltpu.VMEM((DEPTH, GATES), BF16),
                pltpu.VMEM((GATES,), F32),
                pltpu.VMEM((STEPS,) + tile, BF16),
                pltpu.VMEM(tile, BF16),
                pltpu.VMEM((2, (ROWS + 2) * 16, TAP_ROWS), BF16),
                pltpu.VMEM((2, (ROWS + 2) * 16, TAP_ROWS), BF16),
                pltpu.VMEM((STEPS, CHUNKS, CELLS, 4 * LANES), F32),
                pltpu.VMEM((STEPS + 1, CHUNKS, STAGE_ROWS, LANES), F32),
                pltpu.VMEM((fields, ROWS * SEQS, CH), BF16),
                pltpu.VMEM((fields, 2, SEQS, CH), BF16),
                pltpu.VMEM((fields, 2, SEQS, COLS, CH), BF16),
                pltpu.VMEM((fields, ROWS * SEQS, CH), BF16),
                pltpu.VMEM((fields, 2, SEQS, CH), BF16),
                pltpu.SemaphoreType.DMA((13,)),
                pltpu.SemaphoreType.DMA((5,)),
                pltpu.SemaphoreType.DMA((fields, 3)),
            ],
            compiler_params=pltpu.CompilerParams(collective_id=0, has_side_effects=True, vmem_limit_bytes=48 * 2**20),
        )(*(pltpu.with_memory_space_constraint(a, pltpu.HBM) for a in (frames, w_x.reshape(DEPTH, GATES), w_h.reshape(DEPTH, GATES), gate_bias, h_init, c_init)))
        return pl.pallas_call(
            write_out,
            out_shape=(jax.ShapeDtypeStruct(frames.shape, BF16), jax.ShapeDtypeStruct(c_init.shape, F32)),
            in_specs=[vmem, vmem],
            out_specs=(hbm, hbm),
            scratch_shapes=[pltpu.SemaphoreType.DMA((STEPS + 1, SEQS))],
        )(*(pltpu.with_memory_space_constraint(a, pltpu.VMEM) for a in (hidden, cell)))

    return jax.shard_map(local_run, mesh=mesh, in_specs=(frame_spec, P(), P(), P(), state_spec, state_spec), out_specs=(frame_spec, state_spec), check_vma=False)
```

```python
import functools

import jax
import jax.numpy as jnp
from jax import lax
from jax.experimental import pallas as pl
from jax.experimental.pallas import tpu as pltpu
from jax.sharding import PartitionSpec as P

MESH = pl.DeviceIdType.MESH
BF16 = jnp.bfloat16
F32 = jnp.float32

STEPS = 4
SEQS = 2
ROWS = 16
COLS = 8
CH = 384
LANES = 128
CHUNKS = CH // LANES
TAP_ROWS = 3 * CH
DEPTH = 3 * TAP_ROWS
GATES = 4 * CH
CELLS = ROWS * SEQS * COLS
PITCH = 16
GROUPS = (ROWS + 2) * SEQS
STAGE_ROWS = GROUPS * PITCH + 8
OWN = (4,)
VERTICAL = (1, 7)
SIDE = (0, 2, 3, 5, 6, 8)


def sigmoid(value):
    return 0.5 * jnp.tanh(0.5 * value) + 0.5


def halves(source, taps):
    return [(source, tap, k) for tap in taps for k in range(CHUNKS)]


def kernel(
    row_count,
    frames_hbm, wx_hbm, wh_hbm, bias_hbm, h_hbm, c_hbm,
    hidden_out, cell,
    wx, wh, bias, frames, h_start, xtaps, htaps, gates, stage,
    send_col, send_cor, recv_row, recv_col, recv_cor,
    load_sem, send_sem, recv_sem,
):
    row = lax.axis_index("rows")
    col = lax.axis_index("cols")
    other = 1 - col
    has_up = row > 0
    has_down = row < row_count - 1
    inner = jnp.logical_and(has_up, has_down)
    first_col = col == 0

    group_of = {}
    for name in ("frame0", "state", "own_x", "own_h", "frame1", "frames", "cell", "bias", "near_x", "far_x", "last_x", "most_h", "last_h"):
        group_of[name] = load_sem.at[len(group_of)]

    def load(name, queue, pairs):
        for src, dst in pairs:
            pltpu.make_async_copy(src, dst, group_of[name]).start(priority=queue)

    def loaded(name, whole):
        pltpu.make_async_copy(whole, whole, group_of[name]).wait()

    def frame_pairs(times):
        return [(frames_hbm.at[t, s], frames.at[t, :, s]) for t in times for s in range(SEQS)]

    def tap_pairs(src, dst, taps):
        return [(src.at[pl.ds(tap * CH, CH)], dst.at[pl.ds(tap * CH, CH)]) for tap in taps]

    def taps_like(dst, count):
        return dst.at[pl.ds(0, count * CH)]

    load("frame0", 0, frame_pairs([0]))
    load("state", 0, [(h_hbm.at[s], h_start.at[:, s]) for s in range(SEQS)])
    load("own_x", 1, tap_pairs(wx_hbm, wx, OWN))
    load("own_h", 1, tap_pairs(wh_hbm, wh, OWN))
    load("frame1", 0, frame_pairs([1]))
    load("frames", 0, frame_pairs([2, 3]))
    load("cell", 0, [(c_hbm.at[s], cell.at[:, s]) for s in range(SEQS)])
    load("bias", 0, [(bias_hbm, bias)])
    load("near_x", 1, tap_pairs(wx_hbm, wx, VERTICAL))
    load("far_x", 1, tap_pairs(wx_hbm, wx, SIDE[:4]))
    load("last_x", 1, tap_pairs(wx_hbm, wx, SIDE[4:]))
    load("most_h", 1, tap_pairs(wh_hbm, wh, VERTICAL + SIDE[:4]))
    load("last_h", 1, tap_pairs(wh_hbm, wh, SIDE[4:]))

    recv_row[...] = jnp.zeros_like(recv_row)
    recv_cor[...] = jnp.zeros_like(recv_cor)

    barrier = pltpu.get_barrier_semaphore()

    def greet(r, c):
        pl.semaphore_signal(barrier, inc=1, device_id={"rows": r, "cols": c}, device_id_type=MESH)

    greet(row, other)

    @pl.when(has_up)
    def _():
        greet(row - 1, col)
        greet(row - 1, other)

    @pl.when(has_down)
    def _():
        greet(row + 1, col)
        greet(row + 1, other)

    def greeted():
        @pl.when(inner)
        def _():
            pl.semaphore_wait(barrier, 5)

        @pl.when(jnp.logical_not(inner))
        def _():
            pl.semaphore_wait(barrier, 3)

    def tile_ref(field):
        if field < STEPS:
            return frames.at[field]
        return h_start if field == STEPS else hidden_out.at[field - STEPS - 1]

    def field_taps(field):
        return xtaps.at[field] if field < STEPS else htaps.at[field % 2]

    def remote(field, n, src, dst, r, c):
        return pltpu.make_async_remote_copy(
            src_ref=src, dst_ref=dst, send_sem=send_sem.at[n], recv_sem=recv_sem.at[field, (0, 0, 1, 2, 2)[n]],
            device_id={"rows": r, "cols": c}, device_id_type=MESH,
        )

    def copies(field):
        tile = tile_ref(field)
        return dict(
            up=remote(field, 0, tile.at[0], recv_row.at[field, 1], row - 1, col),
            down=remote(field, 1, tile.at[ROWS - 1], recv_row.at[field, 0], row + 1, col),
            side=remote(field, 2, send_col.at[field], recv_col.at[field], row, other),
            up_side=remote(field, 3, send_cor.at[field, 0], recv_cor.at[field, 1], row - 1, other),
            down_side=remote(field, 4, send_cor.at[field, 1], recv_cor.at[field, 0], row + 1, other),
        )

    def send(field):
        out = copies(field)

        @pl.when(has_up)
        def _():
            out["up_side"].start()
            out["up"].start()

        @pl.when(has_down)
        def _():
            out["down_side"].start()
            out["down"].start()

        out["side"].start()

    def pair_arrived(field, n, both):
        @pl.when(inner)
        def _():
            pltpu.make_async_copy(both, both, recv_sem.at[field, n]).wait()

        @pl.when(jnp.logical_not(inner))
        def _():
            pltpu.make_async_copy(both.at[0], both.at[0], recv_sem.at[field, n]).wait()

    def rows_arrived(field):
        pair_arrived(field, 0, recv_row.at[field])

    def sides_arrived(field):
        pltpu.make_async_copy(recv_col.at[field], recv_col.at[field], recv_sem.at[field, 1]).wait()
        pair_arrived(field, 2, recv_cor.at[field])

    def all_sent():
        whole_row, whole_cor = recv_row.at[:, 0], recv_cor.at[:, 0]
        remote(0, 2, recv_col, recv_col, row, other).wait_send()

        @pl.when(has_up)
        def _():
            remote(0, 0, whole_row, whole_row, row - 1, col).wait_send()
            remote(0, 3, whole_cor, whole_cor, row - 1, other).wait_send()

        @pl.when(has_down)
        def _():
            remote(0, 1, whole_row, whole_row, row + 1, col).wait_send()
            remote(0, 4, whole_cor, whole_cor, row + 1, other).wait_send()

    def shift_lanes(d, k):
        return slice(d * CH + k * LANES, d * CH + (k + 1) * LANES)

    def slot_of(field):
        return min(field, STEPS)

    def own_tile(field, values, k):
        slot = slot_of(field)
        for g in range(ROWS * SEQS):
            stage[slot, k, pl.ds((g + SEQS) * PITCH + 8, 8), :] = values[g]
        field_taps(field)[16 : 16 + CELLS, shift_lanes(1, k)] = values.reshape(CELLS, LANES).astype(BF16)
        begin = SEQS * PITCH + 8
        last = stage[slot, k, pl.ds(begin + COLS - 1, ROWS * SEQS, stride=PITCH), :]
        first = stage[slot, k, pl.ds(begin, ROWS * SEQS, stride=PITCH), :]
        edge = jnp.where(first_col, last, first).astype(BF16)
        lanes = pl.ds(k * LANES, LANES)
        send_col[field, :, lanes] = edge
        send_cor[field, 0, :, lanes] = edge[:SEQS]
        send_cor[field, 1, :, lanes] = edge[-SEQS:]

    def prepare(field):
        tile = tile_ref(field)
        for k in range(CHUNKS):
            values = tile[:, :, :, k * LANES : (k + 1) * LANES].astype(F32).reshape(ROWS * SEQS, 8, LANES)
            own_tile(field, values, k)

    def shifted(field, y, d, k):
        slot = slot_of(field)
        pair = [stage[slot, k, pl.ds((y * SEQS + s) * PITCH + 7 + d, 8), :] for s in range(SEQS)]
        field_taps(field)[y * 16 : (y + 1) * 16, shift_lanes(d, k)] = jnp.concatenate(pair, axis=0).astype(BF16)

    def build_rows(field):
        slot = slot_of(field)
        for k in range(CHUNKS):
            lanes = pl.ds(k * LANES, LANES)
            for side, g0 in ((0, 0), (1, GROUPS - SEQS)):
                for s in range(SEQS):
                    stage[slot, k, pl.ds((g0 + s) * PITCH + 8, 8), :] = recv_row[field, side, s, :, lanes].astype(F32)
            for y in (0, ROWS + 1):
                shifted(field, y, 1, k)

    def build_sides(field):
        slot = slot_of(field)
        for k in range(CHUNKS):
            lanes = pl.ds(k * LANES, LANES)
            pieces = ((recv_cor[field, 0, :, lanes], 0, SEQS), (recv_col[field, :, lanes], SEQS, ROWS * SEQS), (recv_cor[field, 1, :, lanes], GROUPS - SEQS, SEQS))
            for value, g0, count in pieces:
                value = value.astype(F32)
                stage[slot, k, pl.ds(g0 * PITCH + 7, count, stride=PITCH), :] = jnp.where(first_col, 0.0, value)
                stage[slot, k, pl.ds(g0 * PITCH + 16, count, stride=PITCH), :] = jnp.where(first_col, value, 0.0)
            for y in range(ROWS + 2):
                shifted(field, y, 0, k)
                shifted(field, y, 2, k)

    def operand(half, t):
        source, tap, k = half
        taps = field_taps(t if source == "x" else STEPS + t)
        dy, dx = divmod(tap, 3)
        return taps[dy * 16 : dy * 16 + CELLS, shift_lanes(dx, k)]

    def weight(half, block):
        source, tap, k = half
        w = wx if source == "x" else wh
        first = tap * CH + k * LANES
        return jnp.concatenate([w[first : first + LANES, g * CH + block * LANES : g * CH + (block + 1) * LANES] for g in range(4)], axis=1)

    def product(t, block, parts):
        lhs = jnp.concatenate([operand(p, t) for p in parts], axis=1)
        rhs = jnp.concatenate([weight(p, block) for p in parts], axis=0)
        return jnp.dot(lhs, rhs, preferred_element_type=F32)

    def cell_update(t, block, sums):
        lanes = slice(block * LANES, (block + 1) * LANES)
        pre = [sums[:, g * LANES : (g + 1) * LANES] + bias[pl.ds(g * CH + block * LANES, LANES)] for g in range(4)]
        shape = (ROWS, SEQS, COLS, LANES)
        c_old = cell[:, :, :, lanes].reshape(CELLS, LANES)
        c_new = sigmoid(pre[1]) * c_old + sigmoid(pre[0]) * jnp.tanh(pre[3])
        h_new = sigmoid(pre[2]) * jnp.tanh(c_new)
        cell[:, :, :, lanes] = c_new.reshape(shape)
        hidden_out[t, :, :, :, lanes] = h_new.reshape(shape).astype(BF16)
        if t + 1 < STEPS:
            own_tile(STEPS + t + 1, h_new.reshape(ROWS * SEQS, 8, LANES), block)

    x_all = halves("x", VERTICAL + SIDE)
    x_own, x_vertical, x_side = (halves("x", taps) for taps in (OWN, VERTICAL, SIDE))
    h_own, h_vertical, h_side = (halves("h", taps) for taps in (OWN, VERTICAL, SIDE))

    def add(t, block, parts):
        gates[t, block] += product(t, block, parts)

    loaded("frame0", frames.at[0])
    prepare(0)
    loaded("state", h_start)
    prepare(STEPS)
    greeted()
    send(0)
    send(STEPS)
    loaded("frame1", frames.at[1])
    prepare(1)
    send(1)
    loaded("own_x", taps_like(wx, 1))
    loaded("frames", frames.at[pl.ds(2, 2)])
    prepare(2)
    prepare(3)
    for t in range(1, STEPS):
        for block in range(CHUNKS):
            gates[t, block] = product(t, block, x_own)
    loaded("own_h", taps_like(wh, 1))
    for block in range(CHUNKS):
        gates[0, block] = product(0, block, x_own + h_own)
    send(2)
    send(3)
    loaded("near_x", taps_like(wx, 2))
    rows_arrived(0)
    build_rows(0)
    for block in range(CHUNKS):
        add(0, block, x_vertical)
    loaded("far_x", taps_like(wx, 4))
    sides_arrived(0)
    build_sides(0)
    for block in range(CHUNKS):
        add(0, block, x_side[:12])
    loaded("last_x", taps_like(wx, 2))
    rows_arrived(1)
    sides_arrived(1)
    for block in range(CHUNKS):
        add(0, block, x_side[12:])
    build_rows(1)
    build_sides(1)
    for block in range(CHUNKS):
        add(1, block, x_all[:12])
    loaded("cell", cell)
    loaded("bias", bias)
    loaded("most_h", taps_like(wh, 6))
    loaded("last_h", taps_like(wh, 2))
    rows_arrived(STEPS)
    sides_arrived(STEPS)
    rows_arrived(2)
    sides_arrived(2)
    build_rows(STEPS)
    build_sides(STEPS)
    build_rows(2)
    build_sides(2)
    for block in range(CHUNKS):
        cell_update(0, block, gates[0, block] + product(0, block, h_vertical + h_side))
    send(STEPS + 1)

    rest = {1: x_all[12:] + h_own, 2: x_all[8:] + h_own, 3: x_all[4:] + h_own}
    ahead = {1: x_all[:8], 2: x_all[:4]}
    for t in range(1, STEPS):
        if t in ahead:
            for block in range(CHUNKS):
                add(t + 1, block, ahead[t])
        for block in range(CHUNKS):
            add(t, block, rest[t])
        rows_arrived(STEPS + t)
        build_rows(STEPS + t)
        for block in range(CHUNKS):
            add(t, block, h_vertical)
        sides_arrived(STEPS + t)
        if t + 1 == STEPS:
            all_sent()
        if t + 2 < STEPS:
            rows_arrived(t + 2)
            sides_arrived(t + 2)
        build_sides(STEPS + t)
        if t + 2 < STEPS:
            build_rows(t + 2)
            build_sides(t + 2)
        for block in range(CHUNKS):
            cell_update(t, block, gates[t, block] + product(t, block, h_side))
        if t + 1 < STEPS:
            send(STEPS + t + 1)


def write_out(hidden, cell, out_hbm, c_out_hbm, sem):
    copies = [pltpu.make_async_copy(hidden.at[t, :, s], out_hbm.at[t, s], sem.at[t, s]) for t in range(STEPS) for s in range(SEQS)]
    copies += [pltpu.make_async_copy(cell.at[:, s], c_out_hbm.at[s], sem.at[STEPS, s]) for s in range(SEQS)]
    for copy in copies:
        copy.start()
    for copy in copies:
        copy.wait()


def solution(mesh):
    row_count = mesh.shape["rows"]
    frame_spec = P(None, "batch", "rows", "cols", None)
    state_spec = P("batch", "rows", "cols", None)

    def local_run(frames, w_x, w_h, gate_bias, h_init, c_init):
        hbm = pl.BlockSpec(memory_space=pltpu.HBM)
        vmem = pl.BlockSpec(memory_space=pltpu.VMEM)
        fields = 2 * STEPS
        tile = (ROWS, SEQS, COLS, CH)

        hidden, cell = pl.pallas_call(
            functools.partial(kernel, row_count),
            out_shape=(pltpu.VMEM((STEPS,) + tile, BF16), pltpu.VMEM(tile, F32)),
            in_specs=[hbm] * 6,
            out_specs=(vmem, vmem),
            scratch_shapes=[
                pltpu.VMEM((DEPTH, GATES), BF16),
                pltpu.VMEM((DEPTH, GATES), BF16),
                pltpu.VMEM((GATES,), F32),
                pltpu.VMEM((STEPS,) + tile, BF16),
                pltpu.VMEM(tile, BF16),
                pltpu.VMEM((STEPS, (ROWS + 2) * 16, TAP_ROWS), BF16),
                pltpu.VMEM((2, (ROWS + 2) * 16, TAP_ROWS), BF16),
                pltpu.VMEM((STEPS, CHUNKS, CELLS, 4 * LANES), F32),
                pltpu.VMEM((STEPS + 1, CHUNKS, STAGE_ROWS, LANES), F32),
                pltpu.VMEM((fields, ROWS * SEQS, CH), BF16),
                pltpu.VMEM((fields, 2, SEQS, CH), BF16),
                pltpu.VMEM((fields, 2, SEQS, COLS, CH), BF16),
                pltpu.VMEM((fields, ROWS * SEQS, CH), BF16),
                pltpu.VMEM((fields, 2, SEQS, CH), BF16),
                pltpu.SemaphoreType.DMA((13,)),
                pltpu.SemaphoreType.DMA((5,)),
                pltpu.SemaphoreType.DMA((fields, 3)),
            ],
            compiler_params=pltpu.CompilerParams(collective_id=0, has_side_effects=True, vmem_limit_bytes=48 * 2**20),
        )(*(pltpu.with_memory_space_constraint(a, pltpu.HBM) for a in (frames, w_x.reshape(DEPTH, GATES), w_h.reshape(DEPTH, GATES), gate_bias, h_init, c_init)))
        return pl.pallas_call(
            write_out,
            out_shape=(jax.ShapeDtypeStruct(frames.shape, BF16), jax.ShapeDtypeStruct(c_init.shape, F32)),
            in_specs=[vmem, vmem],
            out_specs=(hbm, hbm),
            scratch_shapes=[pltpu.SemaphoreType.DMA((STEPS + 1, SEQS))],
        )(*(pltpu.with_memory_space_constraint(a, pltpu.VMEM) for a in (hidden, cell)))

    return jax.shard_map(local_run, mesh=mesh, in_specs=(frame_spec, P(), P(), P(), state_spec, state_spec), out_specs=(frame_spec, state_spec), check_vma=False)
```

```python
import functools

import jax
import jax.numpy as jnp
from jax import lax
from jax.experimental import pallas as pl
from jax.experimental.pallas import tpu as pltpu
from jax.sharding import PartitionSpec as P

MESH = pl.DeviceIdType.MESH
BF16 = jnp.bfloat16
F32 = jnp.float32

STEPS = 4
SEQS = 2
ROWS = 16
COLS = 8
CH = 384
LANES = 128
CHUNKS = CH // LANES
TAP_ROWS = 3 * CH
DEPTH = 3 * TAP_ROWS
GATES = 4 * CH
CELLS = ROWS * SEQS * COLS
PITCH = 16
GROUPS = (ROWS + 2) * SEQS
STAGE_ROWS = GROUPS * PITCH + 8
OWN = (4,)
VERTICAL = (1, 7)
SIDE = (0, 2, 3, 5, 6, 8)


def sigmoid(value):
    return 0.5 * jnp.tanh(0.5 * value) + 0.5


def halves(source, taps):
    return [(source, tap, k) for tap in taps for k in range(CHUNKS)]


def kernel(
    row_count,
    frames_hbm, wx_hbm, wh_hbm, bias_hbm, h_hbm, c_hbm,
    hidden_out, cell,
    wx, wh, bias, frames, h_start, xtaps, htaps, gates, stage,
    send_col, send_cor, recv_row, recv_col, recv_cor,
    load_sem, send_sem, recv_sem,
):
    row = lax.axis_index("rows")
    col = lax.axis_index("cols")
    other = 1 - col
    has_up = row > 0
    has_down = row < row_count - 1
    inner = jnp.logical_and(has_up, has_down)
    first_col = col == 0

    group_of = {}
    for name in ("frame0", "state", "own_x", "own_h", "frame1", "frames", "cell", "bias", "near_x", "far_x", "last_x", "most_h", "last_h"):
        group_of[name] = load_sem.at[len(group_of)]

    def load(name, queue, pairs):
        for src, dst in pairs:
            pltpu.make_async_copy(src, dst, group_of[name]).start(priority=queue)

    def loaded(name, whole):
        pltpu.make_async_copy(whole, whole, group_of[name]).wait()

    def frame_pairs(times):
        return [(frames_hbm.at[t, s], frames.at[t, :, s]) for t in times for s in range(SEQS)]

    def tap_pairs(src, dst, taps):
        return [(src.at[pl.ds(tap * CH, CH)], dst.at[pl.ds(tap * CH, CH)]) for tap in taps]

    def taps_like(dst, count):
        return dst.at[pl.ds(0, count * CH)]

    load("frame0", 0, frame_pairs([0]))
    load("state", 0, [(h_hbm.at[s], h_start.at[:, s]) for s in range(SEQS)])
    load("own_x", 1, tap_pairs(wx_hbm, wx, OWN))
    load("own_h", 1, tap_pairs(wh_hbm, wh, OWN))
    load("frame1", 0, frame_pairs([1]))
    load("frames", 0, frame_pairs([2, 3]))
    load("cell", 0, [(c_hbm.at[s], cell.at[:, s]) for s in range(SEQS)])
    load("bias", 0, [(bias_hbm, bias)])
    load("near_x", 1, tap_pairs(wx_hbm, wx, VERTICAL))
    load("far_x", 1, tap_pairs(wx_hbm, wx, SIDE[:4]))
    load("last_x", 1, tap_pairs(wx_hbm, wx, SIDE[4:]))
    load("most_h", 1, tap_pairs(wh_hbm, wh, VERTICAL + SIDE[:4]))
    load("last_h", 1, tap_pairs(wh_hbm, wh, SIDE[4:]))

    recv_row[...] = jnp.zeros_like(recv_row)
    recv_cor[...] = jnp.zeros_like(recv_cor)

    barrier = pltpu.get_barrier_semaphore()

    def greet(r, c):
        pl.semaphore_signal(barrier, inc=1, device_id={"rows": r, "cols": c}, device_id_type=MESH)

    greet(row, other)

    @pl.when(has_up)
    def _():
        greet(row - 1, col)
        greet(row - 1, other)

    @pl.when(has_down)
    def _():
        greet(row + 1, col)
        greet(row + 1, other)

    def greeted():
        @pl.when(inner)
        def _():
            pl.semaphore_wait(barrier, 5)

        @pl.when(jnp.logical_not(inner))
        def _():
            pl.semaphore_wait(barrier, 3)

    def tile_ref(field):
        if field < STEPS:
            return frames.at[field]
        return h_start if field == STEPS else hidden_out.at[field - STEPS - 1]

    def field_taps(field):
        return xtaps.at[field] if field < STEPS else htaps.at[field % 2]

    def remote(field, n, src, dst, r, c):
        return pltpu.make_async_remote_copy(
            src_ref=src, dst_ref=dst, send_sem=send_sem.at[n], recv_sem=recv_sem.at[field, (0, 0, 1, 2, 2)[n]],
            device_id={"rows": r, "cols": c}, device_id_type=MESH,
        )

    def copies(field):
        tile = tile_ref(field)
        return dict(
            up=remote(field, 0, tile.at[0], recv_row.at[field, 1], row - 1, col),
            down=remote(field, 1, tile.at[ROWS - 1], recv_row.at[field, 0], row + 1, col),
            side=remote(field, 2, send_col.at[field], recv_col.at[field], row, other),
            up_side=remote(field, 3, send_cor.at[field, 0], recv_cor.at[field, 1], row - 1, other),
            down_side=remote(field, 4, send_cor.at[field, 1], recv_cor.at[field, 0], row + 1, other),
        )

    def send(field, names=("up_side", "up", "down_side", "down", "side")):
        out = copies(field)

        @pl.when(has_up)
        def _():
            for name in names:
                if name.startswith("up"):
                    out[name].start()

        @pl.when(has_down)
        def _():
            for name in names:
                if name.startswith("down"):
                    out[name].start()

        if "side" in names:
            out["side"].start()

    def pair_arrived(field, n, both):
        @pl.when(inner)
        def _():
            pltpu.make_async_copy(both, both, recv_sem.at[field, n]).wait()

        @pl.when(jnp.logical_not(inner))
        def _():
            pltpu.make_async_copy(both.at[0], both.at[0], recv_sem.at[field, n]).wait()

    def rows_arrived(field):
        pair_arrived(field, 0, recv_row.at[field])

    def sides_arrived(field):
        pltpu.make_async_copy(recv_col.at[field], recv_col.at[field], recv_sem.at[field, 1]).wait()
        pair_arrived(field, 2, recv_cor.at[field])

    def all_sent():
        whole_row, whole_cor = recv_row.at[:, 0], recv_cor.at[:, 0]
        remote(0, 2, recv_col, recv_col, row, other).wait_send()

        @pl.when(has_up)
        def _():
            remote(0, 0, whole_row, whole_row, row - 1, col).wait_send()
            remote(0, 3, whole_cor, whole_cor, row - 1, other).wait_send()

        @pl.when(has_down)
        def _():
            remote(0, 1, whole_row, whole_row, row + 1, col).wait_send()
            remote(0, 4, whole_cor, whole_cor, row + 1, other).wait_send()

    def shift_lanes(d, k):
        return slice(d * CH + k * LANES, d * CH + (k + 1) * LANES)

    def slot_of(field):
        return min(field, STEPS)

    def own_tile(field, values, k):
        slot = slot_of(field)
        for g in range(ROWS * SEQS):
            stage[slot, k, pl.ds((g + SEQS) * PITCH + 8, 8), :] = values[g]
        field_taps(field)[16 : 16 + CELLS, shift_lanes(1, k)] = values.reshape(CELLS, LANES).astype(BF16)
        begin = SEQS * PITCH + 8
        last = stage[slot, k, pl.ds(begin + COLS - 1, ROWS * SEQS, stride=PITCH), :]
        first = stage[slot, k, pl.ds(begin, ROWS * SEQS, stride=PITCH), :]
        edge = jnp.where(first_col, last, first).astype(BF16)
        lanes = pl.ds(k * LANES, LANES)
        send_col[field, :, lanes] = edge
        send_cor[field, 0, :, lanes] = edge[:SEQS]
        send_cor[field, 1, :, lanes] = edge[-SEQS:]

    def prepare(field):
        tile = tile_ref(field)
        for k in range(CHUNKS):
            values = tile[:, :, :, k * LANES : (k + 1) * LANES].astype(F32).reshape(ROWS * SEQS, 8, LANES)
            own_tile(field, values, k)

    def shifted(field, y, d, k):
        slot = slot_of(field)
        pair = [stage[slot, k, pl.ds((y * SEQS + s) * PITCH + 7 + d, 8), :] for s in range(SEQS)]
        field_taps(field)[y * 16 : (y + 1) * 16, shift_lanes(d, k)] = jnp.concatenate(pair, axis=0).astype(BF16)

    def build_rows(field):
        slot = slot_of(field)
        for k in range(CHUNKS):
            lanes = pl.ds(k * LANES, LANES)
            for side, g0 in ((0, 0), (1, GROUPS - SEQS)):
                for s in range(SEQS):
                    stage[slot, k, pl.ds((g0 + s) * PITCH + 8, 8), :] = recv_row[field, side, s, :, lanes].astype(F32)
            for y in (0, ROWS + 1):
                shifted(field, y, 1, k)

    def build_sides(field):
        slot = slot_of(field)
        for k in range(CHUNKS):
            lanes = pl.ds(k * LANES, LANES)
            pieces = ((recv_cor[field, 0, :, lanes], 0, SEQS), (recv_col[field, :, lanes], SEQS, ROWS * SEQS), (recv_cor[field, 1, :, lanes], GROUPS - SEQS, SEQS))
            for value, g0, count in pieces:
                value = value.astype(F32)
                stage[slot, k, pl.ds(g0 * PITCH + 7, count, stride=PITCH), :] = jnp.where(first_col, 0.0, value)
                stage[slot, k, pl.ds(g0 * PITCH + 16, count, stride=PITCH), :] = jnp.where(first_col, value, 0.0)
            for y in range(ROWS + 2):
                shifted(field, y, 0, k)
                shifted(field, y, 2, k)

    def operand(half, t):
        source, tap, k = half
        taps = field_taps(t if source == "x" else STEPS + t)
        dy, dx = divmod(tap, 3)
        return taps[dy * 16 : dy * 16 + CELLS, shift_lanes(dx, k)]

    def weight(half, block):
        source, tap, k = half
        w = wx if source == "x" else wh
        first = tap * CH + k * LANES
        return jnp.concatenate([w[first : first + LANES, g * CH + block * LANES : g * CH + (block + 1) * LANES] for g in range(4)], axis=1)

    def product(t, block, parts):
        lhs = jnp.concatenate([operand(p, t) for p in parts], axis=1)
        rhs = jnp.concatenate([weight(p, block) for p in parts], axis=0)
        return jnp.dot(lhs, rhs, preferred_element_type=F32)

    def cell_update(t, block, sums):
        lanes = slice(block * LANES, (block + 1) * LANES)
        pre = [sums[:, g * LANES : (g + 1) * LANES] + bias[pl.ds(g * CH + block * LANES, LANES)] for g in range(4)]
        shape = (ROWS, SEQS, COLS, LANES)
        c_old = cell[:, :, :, lanes].reshape(CELLS, LANES)
        c_new = sigmoid(pre[1]) * c_old + sigmoid(pre[0]) * jnp.tanh(pre[3])
        h_new = sigmoid(pre[2]) * jnp.tanh(c_new)
        cell[:, :, :, lanes] = c_new.reshape(shape)
        hidden_out[t, :, :, :, lanes] = h_new.reshape(shape).astype(BF16)
        if t + 1 < STEPS:
            own_tile(STEPS + t + 1, h_new.reshape(ROWS * SEQS, 8, LANES), block)

    x_all = halves("x", VERTICAL + SIDE)
    x_own, x_vertical, x_side = (halves("x", taps) for taps in (OWN, VERTICAL, SIDE))
    h_own, h_vertical, h_side = (halves("h", taps) for taps in (OWN, VERTICAL, SIDE))

    def add(t, block, parts):
        gates[t, block] += product(t, block, parts)

    loaded("frame0", frames.at[0])
    greeted()
    send(0, ("up", "down"))
    prepare(0)
    send(0, ("up_side", "down_side", "side"))
    loaded("state", h_start)
    prepare(STEPS)
    send(STEPS)
    loaded("frame1", frames.at[1])
    prepare(1)
    send(1)
    loaded("frames", frames.at[pl.ds(2, 2)])
    prepare(2)
    send(2)
    prepare(3)
    send(3)
    loaded("own_x", taps_like(wx, 1))
    loaded("own_h", taps_like(wh, 1))
    for t in range(1, STEPS):
        for block in range(CHUNKS):
            gates[t, block] = product(t, block, x_own[:2])
    for block in range(CHUNKS):
        gates[0, block] = product(0, block, x_own + h_own)
    loaded("near_x", taps_like(wx, 2))
    rows_arrived(0)
    build_rows(0)
    for block in range(CHUNKS):
        add(0, block, x_vertical)
    loaded("far_x", taps_like(wx, 4))
    sides_arrived(0)
    build_sides(0)
    for block in range(CHUNKS):
        add(0, block, x_side[:12])
    loaded("last_x", taps_like(wx, 2))
    for t in (1,):
        rows_arrived(t)
        sides_arrived(t)
    for block in range(CHUNKS):
        add(0, block, x_side[12:])
    for t in (1,):
        build_rows(t)
        build_sides(t)
    for block in range(CHUNKS):
        add(1, block, x_all[:12])
    loaded("cell", cell)
    loaded("bias", bias)
    loaded("most_h", taps_like(wh, 6))
    loaded("last_h", taps_like(wh, 2))
    rows_arrived(STEPS)
    sides_arrived(STEPS)
    rows_arrived(2)
    sides_arrived(2)
    build_rows(STEPS)
    build_sides(STEPS)
    build_rows(2)
    build_sides(2)
    for block in range(CHUNKS):
        cell_update(0, block, gates[0, block] + product(0, block, h_vertical + h_side))
    send(STEPS + 1)

    own_rest = x_own[2:] + h_own
    rest = {1: x_all[12:] + own_rest, 2: x_all[8:] + own_rest, 3: x_all[4:] + own_rest}
    ahead = {1: x_all[:8], 2: x_all[:4]}
    for t in range(1, STEPS):
        if t in ahead:
            for block in range(CHUNKS):
                add(t + 1, block, ahead[t])
        for block in range(CHUNKS):
            add(t, block, rest[t])
        rows_arrived(STEPS + t)
        build_rows(STEPS + t)
        for block in range(CHUNKS):
            add(t, block, h_vertical)
        sides_arrived(STEPS + t)
        if t + 1 == STEPS:
            all_sent()
        if t + 2 < STEPS:
            rows_arrived(t + 2)
            sides_arrived(t + 2)
        build_sides(STEPS + t)
        if t + 2 < STEPS:
            build_rows(t + 2)
            build_sides(t + 2)
        for block in range(CHUNKS):
            cell_update(t, block, gates[t, block] + product(t, block, h_side))
        if t + 1 < STEPS:
            send(STEPS + t + 1)


def write_out(hidden, cell, out_hbm, c_out_hbm, sem):
    copies = [pltpu.make_async_copy(hidden.at[t, :, s], out_hbm.at[t, s], sem.at[t, s]) for t in range(STEPS) for s in range(SEQS)]
    copies += [pltpu.make_async_copy(cell.at[:, s], c_out_hbm.at[s], sem.at[STEPS, s]) for s in range(SEQS)]
    for copy in copies:
        copy.start()
    for copy in copies:
        copy.wait()


def solution(mesh):
    row_count = mesh.shape["rows"]
    frame_spec = P(None, "batch", "rows", "cols", None)
    state_spec = P("batch", "rows", "cols", None)

    def local_run(frames, w_x, w_h, gate_bias, h_init, c_init):
        hbm = pl.BlockSpec(memory_space=pltpu.HBM)
        vmem = pl.BlockSpec(memory_space=pltpu.VMEM)
        fields = 2 * STEPS
        tile = (ROWS, SEQS, COLS, CH)

        hidden, cell = pl.pallas_call(
            functools.partial(kernel, row_count),
            out_shape=(pltpu.VMEM((STEPS,) + tile, BF16), pltpu.VMEM(tile, F32)),
            in_specs=[hbm] * 6,
            out_specs=(vmem, vmem),
            scratch_shapes=[
                pltpu.VMEM((DEPTH, GATES), BF16),
                pltpu.VMEM((DEPTH, GATES), BF16),
                pltpu.VMEM((GATES,), F32),
                pltpu.VMEM((STEPS,) + tile, BF16),
                pltpu.VMEM(tile, BF16),
                pltpu.VMEM((STEPS, (ROWS + 2) * 16, TAP_ROWS), BF16),
                pltpu.VMEM((2, (ROWS + 2) * 16, TAP_ROWS), BF16),
                pltpu.VMEM((STEPS, CHUNKS, CELLS, 4 * LANES), F32),
                pltpu.VMEM((STEPS + 1, CHUNKS, STAGE_ROWS, LANES), F32),
                pltpu.VMEM((fields, ROWS * SEQS, CH), BF16),
                pltpu.VMEM((fields, 2, SEQS, CH), BF16),
                pltpu.VMEM((fields, 2, SEQS, COLS, CH), BF16),
                pltpu.VMEM((fields, ROWS * SEQS, CH), BF16),
                pltpu.VMEM((fields, 2, SEQS, CH), BF16),
                pltpu.SemaphoreType.DMA((13,)),
                pltpu.SemaphoreType.DMA((5,)),
                pltpu.SemaphoreType.DMA((fields, 3)),
            ],
            compiler_params=pltpu.CompilerParams(collective_id=0, has_side_effects=True, vmem_limit_bytes=48 * 2**20),
        )(*(pltpu.with_memory_space_constraint(a, pltpu.HBM) for a in (frames, w_x.reshape(DEPTH, GATES), w_h.reshape(DEPTH, GATES), gate_bias, h_init, c_init)))
        return pl.pallas_call(
            write_out,
            out_shape=(jax.ShapeDtypeStruct(frames.shape, BF16), jax.ShapeDtypeStruct(c_init.shape, F32)),
            in_specs=[vmem, vmem],
            out_specs=(hbm, hbm),
            scratch_shapes=[pltpu.SemaphoreType.DMA((STEPS + 1, SEQS))],
        )(*(pltpu.with_memory_space_constraint(a, pltpu.VMEM) for a in (hidden, cell)))

    return jax.shard_map(local_run, mesh=mesh, in_specs=(frame_spec, P(), P(), P(), state_spec, state_spec), out_specs=(frame_spec, state_spec), check_vma=False)
```

```python
import functools

import jax
import jax.numpy as jnp
from jax import lax
from jax.experimental import pallas as pl
from jax.experimental.pallas import tpu as pltpu
from jax.sharding import PartitionSpec as P

MESH = pl.DeviceIdType.MESH
BF16 = jnp.bfloat16
F32 = jnp.float32

STEPS = 4
SEQS = 2
ROWS = 16
COLS = 8
CH = 384
LANES = 128
CHUNKS = CH // LANES
TAP_ROWS = 3 * CH
DEPTH = 3 * TAP_ROWS
GATES = 4 * CH
CELLS = ROWS * SEQS * COLS
PITCH = 16
GROUPS = (ROWS + 2) * SEQS
STAGE_ROWS = GROUPS * PITCH + 8
OWN = (4,)
VERTICAL = (1, 7)
SIDE = (0, 2, 3, 5, 6, 8)


def sigmoid(value):
    return 0.5 * jnp.tanh(0.5 * value) + 0.5


def halves(source, taps):
    return [(source, tap, k) for tap in taps for k in range(CHUNKS)]


def kernel(
    row_count,
    frames_hbm, wx_hbm, wh_hbm, bias_hbm, h_hbm, c_hbm,
    hidden_out, cell,
    wx, wh, bias, frames, h_start, xtaps, htaps, gates, stage,
    send_col, send_cor, recv_row, recv_col, recv_cor,
    load_sem, send_sem, recv_sem,
):
    row = lax.axis_index("rows")
    col = lax.axis_index("cols")
    other = 1 - col
    has_up = row > 0
    has_down = row < row_count - 1
    inner = jnp.logical_and(has_up, has_down)
    first_col = col == 0

    group_of = {}
    for name in ("frame0", "state", "own_x", "own_h", "frame1", "frames", "cell", "bias", "near_x", "far_x", "last_x", "most_h", "last_h"):
        group_of[name] = load_sem.at[len(group_of)]

    def load(name, queue, pairs):
        for src, dst in pairs:
            pltpu.make_async_copy(src, dst, group_of[name]).start(priority=queue)

    def loaded(name, whole):
        pltpu.make_async_copy(whole, whole, group_of[name]).wait()

    def frame_pairs(times):
        return [(frames_hbm.at[t, s], frames.at[t, :, s]) for t in times for s in range(SEQS)]

    def tap_pairs(src, dst, taps):
        return [(src.at[pl.ds(tap * CH, CH)], dst.at[pl.ds(tap * CH, CH)]) for tap in taps]

    def taps_like(dst, count):
        return dst.at[pl.ds(0, count * CH)]

    load("frame0", 0, frame_pairs([0]))
    load("state", 0, [(h_hbm.at[s], h_start.at[:, s]) for s in range(SEQS)])
    load("own_x", 1, tap_pairs(wx_hbm, wx, OWN))
    load("own_h", 1, tap_pairs(wh_hbm, wh, OWN))
    load("frame1", 0, frame_pairs([1]))
    load("frames", 0, frame_pairs([2, 3]))
    load("cell", 0, [(c_hbm.at[s], cell.at[:, s]) for s in range(SEQS)])
    load("bias", 0, [(bias_hbm, bias)])
    load("near_x", 1, tap_pairs(wx_hbm, wx, VERTICAL))
    load("far_x", 1, tap_pairs(wx_hbm, wx, SIDE[:4]))
    load("last_x", 1, tap_pairs(wx_hbm, wx, SIDE[4:]))
    load("most_h", 1, tap_pairs(wh_hbm, wh, VERTICAL + SIDE[:4]))
    load("last_h", 1, tap_pairs(wh_hbm, wh, SIDE[4:]))

    recv_row[...] = jnp.zeros_like(recv_row)
    recv_cor[...] = jnp.zeros_like(recv_cor)

    barrier = pltpu.get_barrier_semaphore()

    def greet(r, c):
        pl.semaphore_signal(barrier, inc=1, device_id={"rows": r, "cols": c}, device_id_type=MESH)

    greet(row, other)

    @pl.when(has_up)
    def _():
        greet(row - 1, col)
        greet(row - 1, other)

    @pl.when(has_down)
    def _():
        greet(row + 1, col)
        greet(row + 1, other)

    def greeted():
        @pl.when(inner)
        def _():
            pl.semaphore_wait(barrier, 5)

        @pl.when(jnp.logical_not(inner))
        def _():
            pl.semaphore_wait(barrier, 3)

    def tile_ref(field):
        if field < STEPS:
            return frames.at[field]
        return h_start if field == STEPS else hidden_out.at[field - STEPS - 1]

    def field_taps(field):
        return xtaps.at[field] if field < STEPS else htaps.at[field % 2]

    def remote(field, n, src, dst, r, c):
        return pltpu.make_async_remote_copy(
            src_ref=src, dst_ref=dst, send_sem=send_sem.at[n], recv_sem=recv_sem.at[field, (0, 0, 1, 2, 2)[n]],
            device_id={"rows": r, "cols": c}, device_id_type=MESH,
        )

    def copies(field):
        tile = tile_ref(field)
        return dict(
            up=remote(field, 0, tile.at[0], recv_row.at[field, 1], row - 1, col),
            down=remote(field, 1, tile.at[ROWS - 1], recv_row.at[field, 0], row + 1, col),
            side=remote(field, 2, send_col.at[field], recv_col.at[field], row, other),
            up_side=remote(field, 3, send_cor.at[field, 0], recv_cor.at[field, 1], row - 1, other),
            down_side=remote(field, 4, send_cor.at[field, 1], recv_cor.at[field, 0], row + 1, other),
        )

    def send(field, names=("up_side", "up", "down_side", "down", "side")):
        out = copies(field)

        @pl.when(has_up)
        def _():
            for name in names:
                if name.startswith("up"):
                    out[name].start()

        @pl.when(has_down)
        def _():
            for name in names:
                if name.startswith("down"):
                    out[name].start()

        if "side" in names:
            out["side"].start()

    def pair_arrived(field, n, both):
        @pl.when(inner)
        def _():
            pltpu.make_async_copy(both, both, recv_sem.at[field, n]).wait()

        @pl.when(jnp.logical_not(inner))
        def _():
            pltpu.make_async_copy(both.at[0], both.at[0], recv_sem.at[field, n]).wait()

    def rows_arrived(field):
        pair_arrived(field, 0, recv_row.at[field])

    def sides_arrived(field):
        pltpu.make_async_copy(recv_col.at[field], recv_col.at[field], recv_sem.at[field, 1]).wait()
        pair_arrived(field, 2, recv_cor.at[field])

    def all_sent():
        whole_row, whole_cor = recv_row.at[:, 0], recv_cor.at[:, 0]
        remote(0, 2, recv_col, recv_col, row, other).wait_send()

        @pl.when(has_up)
        def _():
            remote(0, 0, whole_row, whole_row, row - 1, col).wait_send()
            remote(0, 3, whole_cor, whole_cor, row - 1, other).wait_send()

        @pl.when(has_down)
        def _():
            remote(0, 1, whole_row, whole_row, row + 1, col).wait_send()
            remote(0, 4, whole_cor, whole_cor, row + 1, other).wait_send()

    def shift_lanes(d, k):
        return slice(d * CH + k * LANES, d * CH + (k + 1) * LANES)

    def slot_of(field):
        return min(field, STEPS)

    def own_tile(field, values, k):
        slot = slot_of(field)
        for g in range(ROWS * SEQS):
            stage[slot, k, pl.ds((g + SEQS) * PITCH + 8, 8), :] = values[g]
        field_taps(field)[16 : 16 + CELLS, shift_lanes(1, k)] = values.reshape(CELLS, LANES).astype(BF16)
        begin = SEQS * PITCH + 8
        last = stage[slot, k, pl.ds(begin + COLS - 1, ROWS * SEQS, stride=PITCH), :]
        first = stage[slot, k, pl.ds(begin, ROWS * SEQS, stride=PITCH), :]
        edge = jnp.where(first_col, last, first).astype(BF16)
        lanes = pl.ds(k * LANES, LANES)
        send_col[field, :, lanes] = edge
        send_cor[field, 0, :, lanes] = edge[:SEQS]
        send_cor[field, 1, :, lanes] = edge[-SEQS:]

    def prepare(field):
        tile = tile_ref(field)
        for k in range(CHUNKS):
            values = tile[:, :, :, k * LANES : (k + 1) * LANES].astype(F32).reshape(ROWS * SEQS, 8, LANES)
            own_tile(field, values, k)

    def shifted(field, y, d, k):
        slot = slot_of(field)
        pair = [stage[slot, k, pl.ds((y * SEQS + s) * PITCH + 7 + d, 8), :] for s in range(SEQS)]
        field_taps(field)[y * 16 : (y + 1) * 16, shift_lanes(d, k)] = jnp.concatenate(pair, axis=0).astype(BF16)

    def build_rows(field):
        slot = slot_of(field)
        for k in range(CHUNKS):
            lanes = pl.ds(k * LANES, LANES)
            for side, g0 in ((0, 0), (1, GROUPS - SEQS)):
                for s in range(SEQS):
                    stage[slot, k, pl.ds((g0 + s) * PITCH + 8, 8), :] = recv_row[field, side, s, :, lanes].astype(F32)
            for y in (0, ROWS + 1):
                shifted(field, y, 1, k)

    def build_sides(field):
        slot = slot_of(field)
        for k in range(CHUNKS):
            lanes = pl.ds(k * LANES, LANES)
            pieces = ((recv_cor[field, 0, :, lanes], 0, SEQS), (recv_col[field, :, lanes], SEQS, ROWS * SEQS), (recv_cor[field, 1, :, lanes], GROUPS - SEQS, SEQS))
            for value, g0, count in pieces:
                value = value.astype(F32)
                stage[slot, k, pl.ds(g0 * PITCH + 7, count, stride=PITCH), :] = jnp.where(first_col, 0.0, value)
                stage[slot, k, pl.ds(g0 * PITCH + 16, count, stride=PITCH), :] = jnp.where(first_col, value, 0.0)
            for y in range(ROWS + 2):
                shifted(field, y, 0, k)
                shifted(field, y, 2, k)

    def operand(half, t):
        source, tap, k = half
        taps = field_taps(t if source == "x" else STEPS + t)
        dy, dx = divmod(tap, 3)
        return taps[dy * 16 : dy * 16 + CELLS, shift_lanes(dx, k)]

    def weight(half, block):
        source, tap, k = half
        w = wx if source == "x" else wh
        first = tap * CH + k * LANES
        return jnp.concatenate([w[first : first + LANES, g * CH + block * LANES : g * CH + (block + 1) * LANES] for g in range(4)], axis=1)

    def product(t, block, parts):
        lhs = jnp.concatenate([operand(p, t) for p in parts], axis=1)
        rhs = jnp.concatenate([weight(p, block) for p in parts], axis=0)
        return jnp.dot(lhs, rhs, preferred_element_type=F32)

    def cell_update(t, block, sums):
        lanes = slice(block * LANES, (block + 1) * LANES)
        pre = [sums[:, g * LANES : (g + 1) * LANES] + bias[pl.ds(g * CH + block * LANES, LANES)] for g in range(4)]
        shape = (ROWS, SEQS, COLS, LANES)
        c_old = cell[:, :, :, lanes].reshape(CELLS, LANES)
        c_new = sigmoid(pre[1]) * c_old + sigmoid(pre[0]) * jnp.tanh(pre[3])
        h_new = sigmoid(pre[2]) * jnp.tanh(c_new)
        cell[:, :, :, lanes] = c_new.reshape(shape)
        hidden_out[t, :, :, :, lanes] = h_new.reshape(shape).astype(BF16)
        if t + 1 < STEPS:
            own_tile(STEPS + t + 1, h_new.reshape(ROWS * SEQS, 8, LANES), block)

    x_all = halves("x", VERTICAL + SIDE)
    x_own, x_vertical, x_side = (halves("x", taps) for taps in (OWN, VERTICAL, SIDE))
    h_own, h_vertical, h_side = (halves("h", taps) for taps in (OWN, VERTICAL, SIDE))

    def add(t, block, parts):
        gates[t, block] += product(t, block, parts)

    loaded("frame0", frames.at[0])
    greeted()
    send(0, ("up", "down"))
    prepare(0)
    send(0, ("up_side", "down_side", "side"))
    loaded("state", h_start)
    prepare(STEPS)
    send(STEPS)
    loaded("frame1", frames.at[1])
    prepare(1)
    send(1)
    loaded("frames", frames.at[pl.ds(2, 2)])
    prepare(2)
    send(2)
    prepare(3)
    send(3)
    loaded("own_x", taps_like(wx, 1))
    loaded("own_h", taps_like(wh, 1))
    for t in range(1, STEPS):
        for block in range(CHUNKS):
            gates[t, block] = product(t, block, x_own[:2])
    for block in range(CHUNKS):
        gates[0, block] = product(0, block, x_own + h_own)
    loaded("near_x", taps_like(wx, 2))
    rows_arrived(0)
    build_rows(0)
    for block in range(CHUNKS):
        add(0, block, x_vertical)
    loaded("far_x", taps_like(wx, 4))
    sides_arrived(0)
    build_sides(0)
    for block in range(CHUNKS):
        add(0, block, x_side[:12])
    loaded("last_x", taps_like(wx, 2))
    for t in (1,):
        rows_arrived(t)
        sides_arrived(t)
    for block in range(CHUNKS):
        add(0, block, x_side[12:])
    for t in (1,):
        build_rows(t)
        build_sides(t)
    for block in range(CHUNKS):
        add(1, block, x_all[:12])
    loaded("cell", cell)
    loaded("bias", bias)
    loaded("most_h", taps_like(wh, 6))
    loaded("last_h", taps_like(wh, 2))
    rows_arrived(STEPS)
    sides_arrived(STEPS)
    rows_arrived(2)
    sides_arrived(2)
    build_rows(STEPS)
    build_sides(STEPS)
    build_rows(2)
    build_sides(2)
    for block in range(CHUNKS):
        cell_update(0, block, gates[0, block] + product(0, block, h_vertical + h_side))
    send(STEPS + 1)

    own_rest = x_own[2:] + h_own
    rest = {1: x_all[12:] + own_rest, 2: x_all[8:] + own_rest, 3: x_all[4:] + own_rest}
    ahead = {1: x_all[:8], 2: x_all[:4]}
    for t in range(1, STEPS):
        if t in ahead:
            for block in range(CHUNKS):
                add(t + 1, block, ahead[t])
        for block in range(CHUNKS):
            add(t, block, rest[t])
        rows_arrived(STEPS + t)
        build_rows(STEPS + t)
        for block in range(CHUNKS):
            add(t, block, h_vertical)
        sides_arrived(STEPS + t)
        if t + 1 == STEPS:
            all_sent()
        if t + 2 < STEPS:
            rows_arrived(t + 2)
            sides_arrived(t + 2)
        build_sides(STEPS + t)
        if t + 2 < STEPS:
            build_rows(t + 2)
            build_sides(t + 2)
        for block in range(CHUNKS):
            cell_update(t, block, gates[t, block] + product(t, block, h_side))
        if t + 1 < STEPS:
            send(STEPS + t + 1)


def write_out(hidden, cell, out_hbm, c_out_hbm, sem):
    for s in range(SEQS):
        pltpu.make_async_copy(cell.at[:, s], c_out_hbm.at[s], sem.at[0]).start(priority=s)
    for t in range(STEPS):
        for s in range(SEQS):
            pltpu.make_async_copy(hidden.at[t, :, s], out_hbm.at[t, s], sem.at[1]).start(priority=s)
    pltpu.make_async_copy(cell, cell, sem.at[0]).wait()
    pltpu.make_async_copy(hidden, hidden, sem.at[1]).wait()


def solution(mesh):
    row_count = mesh.shape["rows"]
    frame_spec = P(None, "batch", "rows", "cols", None)
    state_spec = P("batch", "rows", "cols", None)

    def local_run(frames, w_x, w_h, gate_bias, h_init, c_init):
        hbm = pl.BlockSpec(memory_space=pltpu.HBM)
        vmem = pl.BlockSpec(memory_space=pltpu.VMEM)
        fields = 2 * STEPS
        tile = (ROWS, SEQS, COLS, CH)

        hidden, cell = pl.pallas_call(
            functools.partial(kernel, row_count),
            out_shape=(pltpu.VMEM((STEPS,) + tile, BF16), pltpu.VMEM(tile, F32)),
            in_specs=[hbm] * 6,
            out_specs=(vmem, vmem),
            scratch_shapes=[
                pltpu.VMEM((DEPTH, GATES), BF16),
                pltpu.VMEM((DEPTH, GATES), BF16),
                pltpu.VMEM((GATES,), F32),
                pltpu.VMEM((STEPS,) + tile, BF16),
                pltpu.VMEM(tile, BF16),
                pltpu.VMEM((STEPS, (ROWS + 2) * 16, TAP_ROWS), BF16),
                pltpu.VMEM((2, (ROWS + 2) * 16, TAP_ROWS), BF16),
                pltpu.VMEM((STEPS, CHUNKS, CELLS, 4 * LANES), F32),
                pltpu.VMEM((STEPS + 1, CHUNKS, STAGE_ROWS, LANES), F32),
                pltpu.VMEM((fields, ROWS * SEQS, CH), BF16),
                pltpu.VMEM((fields, 2, SEQS, CH), BF16),
                pltpu.VMEM((fields, 2, SEQS, COLS, CH), BF16),
                pltpu.VMEM((fields, ROWS * SEQS, CH), BF16),
                pltpu.VMEM((fields, 2, SEQS, CH), BF16),
                pltpu.SemaphoreType.DMA((13,)),
                pltpu.SemaphoreType.DMA((5,)),
                pltpu.SemaphoreType.DMA((fields, 3)),
            ],
            compiler_params=pltpu.CompilerParams(collective_id=0, has_side_effects=True, vmem_limit_bytes=48 * 2**20),
        )(*(pltpu.with_memory_space_constraint(a, pltpu.HBM) for a in (frames, w_x.reshape(DEPTH, GATES), w_h.reshape(DEPTH, GATES), gate_bias, h_init, c_init)))
        return pl.pallas_call(
            write_out,
            out_shape=(jax.ShapeDtypeStruct(frames.shape, BF16), jax.ShapeDtypeStruct(c_init.shape, F32)),
            in_specs=[vmem, vmem],
            out_specs=(hbm, hbm),
            scratch_shapes=[pltpu.SemaphoreType.DMA((2,))],
        )(*(pltpu.with_memory_space_constraint(a, pltpu.VMEM) for a in (hidden, cell)))

    return jax.shard_map(local_run, mesh=mesh, in_specs=(frame_spec, P(), P(), P(), state_spec, state_spec), out_specs=(frame_spec, state_spec), check_vma=False)
```

```python
import functools

import jax
import jax.numpy as jnp
from jax import lax
from jax.experimental import pallas as pl
from jax.experimental.pallas import tpu as pltpu
from jax.sharding import PartitionSpec as P

MESH = pl.DeviceIdType.MESH
BF16 = jnp.bfloat16
F32 = jnp.float32

STEPS = 4
SEQS = 2
ROWS = 16
COLS = 8
CH = 384
LANES = 128
CHUNKS = CH // LANES
TAP_ROWS = 3 * CH
DEPTH = 3 * TAP_ROWS
GATES = 4 * CH
CELLS = ROWS * SEQS * COLS
PITCH = 16
GROUPS = (ROWS + 2) * SEQS
STAGE_ROWS = GROUPS * PITCH + 8
OWN = (4,)
VERTICAL = (1, 7)
SIDE = (0, 2, 3, 5, 6, 8)


def sigmoid(value):
    return 0.5 * jnp.tanh(0.5 * value) + 0.5


def halves(source, taps):
    return [(source, tap, k) for tap in taps for k in range(CHUNKS)]


def kernel(
    row_count,
    frames_hbm, wx_hbm, wh_hbm, bias_hbm, h_hbm, c_hbm,
    hidden_out, cell,
    wx, wh, bias, frames, h_start, xtaps, htaps, gates, stage,
    send_col, send_cor, recv_row, recv_col, recv_cor,
    load_sem, send_sem, recv_sem,
):
    row = lax.axis_index("rows")
    col = lax.axis_index("cols")
    other = 1 - col
    has_up = row > 0
    has_down = row < row_count - 1
    inner = jnp.logical_and(has_up, has_down)
    first_col = col == 0

    group_of = {}
    for name in ("frame0", "state", "own_x", "own_h", "frame1", "frames", "cell", "bias", "near_x", "far_x", "last_x", "most_h", "last_h"):
        group_of[name] = load_sem.at[len(group_of)]

    def load(name, queue, pairs):
        for src, dst in pairs:
            pltpu.make_async_copy(src, dst, group_of[name]).start(priority=queue)

    def loaded(name, whole):
        pltpu.make_async_copy(whole, whole, group_of[name]).wait()

    def frame_pairs(times):
        return [(frames_hbm.at[t, s], frames.at[t, :, s]) for t in times for s in range(SEQS)]

    def tap_pairs(src, dst, taps):
        return [(src.at[pl.ds(tap * CH, CH)], dst.at[pl.ds(tap * CH, CH)]) for tap in taps]

    def taps_like(dst, count):
        return dst.at[pl.ds(0, count * CH)]

    load("frame0", 0, frame_pairs([0]))
    load("state", 0, [(h_hbm.at[s], h_start.at[:, s]) for s in range(SEQS)])
    load("own_x", 1, tap_pairs(wx_hbm, wx, OWN))
    load("own_h", 1, tap_pairs(wh_hbm, wh, OWN))
    load("frame1", 0, frame_pairs([1]))
    load("frames", 0, frame_pairs([2, 3]))
    load("cell", 0, [(c_hbm.at[s], cell.at[:, s]) for s in range(SEQS)])
    load("bias", 0, [(bias_hbm, bias)])
    load("near_x", 1, tap_pairs(wx_hbm, wx, VERTICAL))
    load("far_x", 1, tap_pairs(wx_hbm, wx, SIDE[:4]))
    load("last_x", 1, tap_pairs(wx_hbm, wx, SIDE[4:]))
    load("most_h", 1, tap_pairs(wh_hbm, wh, VERTICAL + SIDE[:4]))
    load("last_h", 1, tap_pairs(wh_hbm, wh, SIDE[4:]))

    recv_row[...] = jnp.zeros_like(recv_row)
    recv_cor[...] = jnp.zeros_like(recv_cor)

    barrier = pltpu.get_barrier_semaphore()

    def greet(r, c):
        pl.semaphore_signal(barrier, inc=1, device_id={"rows": r, "cols": c}, device_id_type=MESH)

    greet(row, other)

    @pl.when(has_up)
    def _():
        greet(row - 1, col)
        greet(row - 1, other)

    @pl.when(has_down)
    def _():
        greet(row + 1, col)
        greet(row + 1, other)

    def greeted():
        @pl.when(inner)
        def _():
            pl.semaphore_wait(barrier, 5)

        @pl.when(jnp.logical_not(inner))
        def _():
            pl.semaphore_wait(barrier, 3)

    def tile_ref(field):
        if field < STEPS:
            return frames.at[field]
        return h_start if field == STEPS else hidden_out.at[field - STEPS - 1]

    def field_taps(field):
        return xtaps.at[field] if field < STEPS else htaps.at[field % 2]

    def remote(field, n, src, dst, r, c):
        return pltpu.make_async_remote_copy(
            src_ref=src, dst_ref=dst, send_sem=send_sem.at[n], recv_sem=recv_sem.at[field, (0, 0, 1, 2, 2)[n]],
            device_id={"rows": r, "cols": c}, device_id_type=MESH,
        )

    def copies(field):
        tile = tile_ref(field)
        return dict(
            up=remote(field, 0, tile.at[0], recv_row.at[field, 1], row - 1, col),
            down=remote(field, 1, tile.at[ROWS - 1], recv_row.at[field, 0], row + 1, col),
            side=remote(field, 2, send_col.at[field], recv_col.at[field], row, other),
            up_side=remote(field, 3, send_cor.at[field, 0], recv_cor.at[field, 1], row - 1, other),
            down_side=remote(field, 4, send_cor.at[field, 1], recv_cor.at[field, 0], row + 1, other),
        )

    def send(field, names=("up_side", "up", "down_side", "down", "side")):
        out = copies(field)
        if "side" in names:
            out["side"].start()

        @pl.when(has_up)
        def _():
            for name in names:
                if name.startswith("up"):
                    out[name].start()

        @pl.when(has_down)
        def _():
            for name in names:
                if name.startswith("down"):
                    out[name].start()


    def pair_arrived(field, n, both):
        @pl.when(inner)
        def _():
            pltpu.make_async_copy(both, both, recv_sem.at[field, n]).wait()

        @pl.when(jnp.logical_not(inner))
        def _():
            pltpu.make_async_copy(both.at[0], both.at[0], recv_sem.at[field, n]).wait()

    def rows_arrived(field):
        pair_arrived(field, 0, recv_row.at[field])

    def sides_arrived(field):
        pltpu.make_async_copy(recv_col.at[field], recv_col.at[field], recv_sem.at[field, 1]).wait()
        pair_arrived(field, 2, recv_cor.at[field])

    def all_sent():
        whole_row, whole_cor = recv_row.at[:, 0], recv_cor.at[:, 0]
        remote(0, 2, recv_col, recv_col, row, other).wait_send()

        @pl.when(has_up)
        def _():
            remote(0, 0, whole_row, whole_row, row - 1, col).wait_send()
            remote(0, 3, whole_cor, whole_cor, row - 1, other).wait_send()

        @pl.when(has_down)
        def _():
            remote(0, 1, whole_row, whole_row, row + 1, col).wait_send()
            remote(0, 4, whole_cor, whole_cor, row + 1, other).wait_send()

    def shift_lanes(d, k):
        return slice(d * CH + k * LANES, d * CH + (k + 1) * LANES)

    def slot_of(field):
        return min(field, STEPS)

    def own_tile(field, values, k):
        slot = slot_of(field)
        for g in range(ROWS * SEQS):
            stage[slot, k, pl.ds((g + SEQS) * PITCH + 8, 8), :] = values[g]
        field_taps(field)[16 : 16 + CELLS, shift_lanes(1, k)] = values.reshape(CELLS, LANES).astype(BF16)
        begin = SEQS * PITCH + 8
        last = stage[slot, k, pl.ds(begin + COLS - 1, ROWS * SEQS, stride=PITCH), :]
        first = stage[slot, k, pl.ds(begin, ROWS * SEQS, stride=PITCH), :]
        edge = jnp.where(first_col, last, first).astype(BF16)
        lanes = pl.ds(k * LANES, LANES)
        send_col[field, :, lanes] = edge
        send_cor[field, 0, :, lanes] = edge[:SEQS]
        send_cor[field, 1, :, lanes] = edge[-SEQS:]

    def prepare(field):
        tile = tile_ref(field)
        for k in range(CHUNKS):
            values = tile[:, :, :, k * LANES : (k + 1) * LANES].astype(F32).reshape(ROWS * SEQS, 8, LANES)
            own_tile(field, values, k)

    def shifted(field, y, d, k):
        slot = slot_of(field)
        pair = [stage[slot, k, pl.ds((y * SEQS + s) * PITCH + 7 + d, 8), :] for s in range(SEQS)]
        field_taps(field)[y * 16 : (y + 1) * 16, shift_lanes(d, k)] = jnp.concatenate(pair, axis=0).astype(BF16)

    def build_rows(field):
        slot = slot_of(field)
        for k in range(CHUNKS):
            lanes = pl.ds(k * LANES, LANES)
            for side, g0 in ((0, 0), (1, GROUPS - SEQS)):
                for s in range(SEQS):
                    stage[slot, k, pl.ds((g0 + s) * PITCH + 8, 8), :] = recv_row[field, side, s, :, lanes].astype(F32)
            for y in (0, ROWS + 1):
                shifted(field, y, 1, k)

    def build_sides(field):
        slot = slot_of(field)
        for k in range(CHUNKS):
            lanes = pl.ds(k * LANES, LANES)
            pieces = ((recv_cor[field, 0, :, lanes], 0, SEQS), (recv_col[field, :, lanes], SEQS, ROWS * SEQS), (recv_cor[field, 1, :, lanes], GROUPS - SEQS, SEQS))
            for value, g0, count in pieces:
                value = value.astype(F32)
                stage[slot, k, pl.ds(g0 * PITCH + 7, count, stride=PITCH), :] = jnp.where(first_col, 0.0, value)
                stage[slot, k, pl.ds(g0 * PITCH + 16, count, stride=PITCH), :] = jnp.where(first_col, value, 0.0)
            for y in range(ROWS + 2):
                shifted(field, y, 0, k)
                shifted(field, y, 2, k)

    def operand(half, t):
        source, tap, k = half
        taps = field_taps(t if source == "x" else STEPS + t)
        dy, dx = divmod(tap, 3)
        return taps[dy * 16 : dy * 16 + CELLS, shift_lanes(dx, k)]

    def weight(half, block):
        source, tap, k = half
        w = wx if source == "x" else wh
        first = tap * CH + k * LANES
        return jnp.concatenate([w[first : first + LANES, g * CH + block * LANES : g * CH + (block + 1) * LANES] for g in range(4)], axis=1)

    def product(t, block, parts):
        lhs = jnp.concatenate([operand(p, t) for p in parts], axis=1)
        rhs = jnp.concatenate([weight(p, block) for p in parts], axis=0)
        return jnp.dot(lhs, rhs, preferred_element_type=F32)

    def cell_update(t, block, sums):
        lanes = slice(block * LANES, (block + 1) * LANES)
        pre = [sums[:, g * LANES : (g + 1) * LANES] + bias[pl.ds(g * CH + block * LANES, LANES)] for g in range(4)]
        shape = (ROWS, SEQS, COLS, LANES)
        c_old = cell[:, :, :, lanes].reshape(CELLS, LANES)
        c_new = sigmoid(pre[1]) * c_old + sigmoid(pre[0]) * jnp.tanh(pre[3])
        h_new = sigmoid(pre[2]) * jnp.tanh(c_new)
        cell[:, :, :, lanes] = c_new.reshape(shape)
        hidden_out[t, :, :, :, lanes] = h_new.reshape(shape).astype(BF16)
        if t + 1 < STEPS:
            own_tile(STEPS + t + 1, h_new.reshape(ROWS * SEQS, 8, LANES), block)

    x_all = halves("x", VERTICAL + SIDE)
    x_own, x_vertical, x_side = (halves("x", taps) for taps in (OWN, VERTICAL, SIDE))
    h_own, h_vertical, h_side = (halves("h", taps) for taps in (OWN, VERTICAL, SIDE))

    def add(t, block, parts):
        gates[t, block] += product(t, block, parts)

    loaded("frame0", frames.at[0])
    greeted()
    send(0, ("up", "down"))
    prepare(0)
    send(0, ("up_side", "down_side", "side"))
    loaded("state", h_start)
    prepare(STEPS)
    send(STEPS)
    loaded("frame1", frames.at[1])
    prepare(1)
    send(1)
    loaded("frames", frames.at[pl.ds(2, 2)])
    prepare(2)
    send(2)
    prepare(3)
    send(3)
    loaded("own_x", taps_like(wx, 1))
    loaded("own_h", taps_like(wh, 1))
    for t in range(1, STEPS):
        for block in range(CHUNKS):
            gates[t, block] = product(t, block, x_own[:2])
    for block in range(CHUNKS):
        gates[0, block] = product(0, block, x_own + h_own)
    loaded("near_x", taps_like(wx, 2))
    rows_arrived(0)
    build_rows(0)
    for block in range(CHUNKS):
        add(0, block, x_vertical)
    loaded("far_x", taps_like(wx, 4))
    sides_arrived(0)
    build_sides(0)
    for block in range(CHUNKS):
        add(0, block, x_side[:12])
    loaded("last_x", taps_like(wx, 2))
    for t in (1,):
        rows_arrived(t)
        sides_arrived(t)
    for block in range(CHUNKS):
        add(0, block, x_side[12:])
    for t in (1,):
        build_rows(t)
        build_sides(t)
    for block in range(CHUNKS):
        add(1, block, x_all[:12])
    loaded("cell", cell)
    loaded("bias", bias)
    loaded("most_h", taps_like(wh, 6))
    loaded("last_h", taps_like(wh, 2))
    rows_arrived(STEPS)
    sides_arrived(STEPS)
    rows_arrived(2)
    sides_arrived(2)
    build_rows(STEPS)
    build_sides(STEPS)
    build_rows(2)
    build_sides(2)
    for block in range(CHUNKS):
        cell_update(0, block, gates[0, block] + product(0, block, h_vertical + h_side))
    send(STEPS + 1)

    own_rest = x_own[2:] + h_own
    rest = {1: x_all[12:] + own_rest, 2: x_all[8:] + own_rest, 3: x_all[4:] + own_rest}
    ahead = {1: x_all[:8], 2: x_all[:4]}
    for t in range(1, STEPS):
        if t in ahead:
            for block in range(CHUNKS):
                add(t + 1, block, ahead[t])
        for block in range(CHUNKS):
            add(t, block, rest[t])
        rows_arrived(STEPS + t)
        build_rows(STEPS + t)
        for block in range(CHUNKS):
            add(t, block, h_vertical)
        sides_arrived(STEPS + t)
        if t + 1 == STEPS:
            all_sent()
        if t + 2 < STEPS:
            rows_arrived(t + 2)
            sides_arrived(t + 2)
        build_sides(STEPS + t)
        if t + 2 < STEPS:
            build_rows(t + 2)
            build_sides(t + 2)
        for block in range(CHUNKS):
            cell_update(t, block, gates[t, block] + product(t, block, h_side))
        if t + 1 < STEPS:
            send(STEPS + t + 1)


def write_out(hidden, cell, out_hbm, c_out_hbm, sem):
    for s in range(SEQS):
        pltpu.make_async_copy(cell.at[:, s], c_out_hbm.at[s], sem.at[0]).start(priority=s)
    for t in range(STEPS):
        for s in range(SEQS):
            pltpu.make_async_copy(hidden.at[t, :, s], out_hbm.at[t, s], sem.at[1]).start(priority=s)
    pltpu.make_async_copy(cell, cell, sem.at[0]).wait()
    pltpu.make_async_copy(hidden, hidden, sem.at[1]).wait()


def solution(mesh):
    row_count = mesh.shape["rows"]
    frame_spec = P(None, "batch", "rows", "cols", None)
    state_spec = P("batch", "rows", "cols", None)

    def local_run(frames, w_x, w_h, gate_bias, h_init, c_init):
        hbm = pl.BlockSpec(memory_space=pltpu.HBM)
        vmem = pl.BlockSpec(memory_space=pltpu.VMEM)
        fields = 2 * STEPS
        tile = (ROWS, SEQS, COLS, CH)

        hidden, cell = pl.pallas_call(
            functools.partial(kernel, row_count),
            out_shape=(pltpu.VMEM((STEPS,) + tile, BF16), pltpu.VMEM(tile, F32)),
            in_specs=[hbm] * 6,
            out_specs=(vmem, vmem),
            scratch_shapes=[
                pltpu.VMEM((DEPTH, GATES), BF16),
                pltpu.VMEM((DEPTH, GATES), BF16),
                pltpu.VMEM((GATES,), F32),
                pltpu.VMEM((STEPS,) + tile, BF16),
                pltpu.VMEM(tile, BF16),
                pltpu.VMEM((STEPS, (ROWS + 2) * 16, TAP_ROWS), BF16),
                pltpu.VMEM((2, (ROWS + 2) * 16, TAP_ROWS), BF16),
                pltpu.VMEM((STEPS, CHUNKS, CELLS, 4 * LANES), F32),
                pltpu.VMEM((STEPS + 1, CHUNKS, STAGE_ROWS, LANES), F32),
                pltpu.VMEM((fields, ROWS * SEQS, CH), BF16),
                pltpu.VMEM((fields, 2, SEQS, CH), BF16),
                pltpu.VMEM((fields, 2, SEQS, COLS, CH), BF16),
                pltpu.VMEM((fields, ROWS * SEQS, CH), BF16),
                pltpu.VMEM((fields, 2, SEQS, CH), BF16),
                pltpu.SemaphoreType.DMA((13,)),
                pltpu.SemaphoreType.DMA((5,)),
                pltpu.SemaphoreType.DMA((fields, 3)),
            ],
            compiler_params=pltpu.CompilerParams(collective_id=0, has_side_effects=True, vmem_limit_bytes=48 * 2**20),
        )(*(pltpu.with_memory_space_constraint(a, pltpu.HBM) for a in (frames, w_x.reshape(DEPTH, GATES), w_h.reshape(DEPTH, GATES), gate_bias, h_init, c_init)))
        return pl.pallas_call(
            write_out,
            out_shape=(jax.ShapeDtypeStruct(frames.shape, BF16), jax.ShapeDtypeStruct(c_init.shape, F32)),
            in_specs=[vmem, vmem],
            out_specs=(hbm, hbm),
            scratch_shapes=[pltpu.SemaphoreType.DMA((2,))],
        )(*(pltpu.with_memory_space_constraint(a, pltpu.VMEM) for a in (hidden, cell)))

    return jax.shard_map(local_run, mesh=mesh, in_specs=(frame_spec, P(), P(), P(), state_spec, state_spec), out_specs=(frame_spec, state_spec), check_vma=False)
```
